256 devices in a mesh: grid: 64 (over x, z, core), chan: 4 (over y).
Axes of the slice: x: 4, y: 4, z: 8, core: 2. Of those that a mesh axis runs over, the one named last changes fastest.
Arguments:
- volt: float32 [2, 128, 4096, 512], P(None, None, 'grid', 'chan'), may hold values from -13 to 13
- placement: int32 [4096], P('grid'), may hold values from 0 to 63, as said below
- flags: int32 [4096], P('grid'), may hold values 0 or 1
Outputs:
- sky_image: float32 [64, 64], P('chan', 'grid')
The draws below stay inside these ranges and needn't reach their ends.
Inputs may be any that keep to these rules, and one draw needn't show every extreme that they name: `placement`: within every grid row r, antennas r * 64 to (r + 1) * 64 - 1 take each column 0 to 63 exactly once.
All inputs are finite; a program needn't handle non-finite values. No bound on the sum of `flags` on one device may be relied on, other than what follows from the above.
Results may differ from the reference program's by a relative error of at most 0.0001.
Values sent between devices are 32-bit elements; how exact they have to be, the bound alone decides.
A program may use at most 128 MiB of HBM per device.

```python
import math
import jax
import jax.numpy as jnp
from jax import lax

NROW = 64
GRID_COLUMNS = 64
CHANNELS = 512
TIMES = 128
ANTENNAS = 4096


source_count = 16


def place_map(key):
    row_keys = jax.random.split(jax.random.fold_in(key, 7), NROW)
    row_perm = jax.vmap(lambda row_key: jax.random.permutation(row_key, GRID_COLUMNS))(row_keys)
    return row_perm.astype(jnp.int32).reshape(ANTENNAS)


def draw_placement(key, part):
    return place_map(key)


def draw_volt(key, part):
    place_col = place_map(key)
    grid_row = jnp.arange(ANTENNAS, dtype=jnp.int32) // GRID_COLUMNS
    base = jax.random.fold_in(key, 9)
    key_row, key_col, key_amp, key_sig, key_noise = jax.random.split(base, 5)
    src_row = jax.random.randint(key_row, (source_count,), 0, NROW)
    src_col = jax.random.randint(key_col, (source_count,), 0, GRID_COLUMNS)
    src_amp = jnp.exp(jax.random.uniform(key_amp, (source_count,), jnp.float32, math.log(0.03), math.log(0.1)))
    src_signal = jnp.clip(jax.random.normal(key_sig, (2, TIMES, CHANNELS, source_count), jnp.float32), -4.0, 4.0)
    src_signal = src_signal * (src_amp / math.sqrt(2.0))
    row_part = (grid_row[:, None] * src_row[None, :] % NROW).astype(jnp.float32) / NROW
    col_part = (place_col[:, None] * src_col[None, :] % GRID_COLUMNS).astype(jnp.float32) / GRID_COLUMNS
    src_phase = 2.0 * math.pi * (row_part + col_part)
    phase_cosine = jnp.cos(src_phase)
    phase_sine = jnp.sin(src_phase)
    signal_real = src_signal[0]
    signal_imaginary = src_signal[1]
    real_component = jnp.einsum('ybd,zd->yzb', signal_real, phase_cosine) - jnp.einsum('ybd,zd->yzb', signal_imaginary, phase_sine)
    imaginary_component = jnp.einsum('ybd,zd->yzb', signal_real, phase_sine) + jnp.einsum('ybd,zd->yzb', signal_imaginary, phase_cosine)
    noise_part = jnp.clip(jax.random.normal(key_noise, (2, TIMES, ANTENNAS, CHANNELS), jnp.float32), -6.0, 6.0)
    return (jnp.stack([real_component, imaginary_component]) + noise_part).astype(jnp.float32)


def place_ends(values, rng, least, largest):
    spot = [jax.random.randint(jax.random.fold_in(rng, axis), (), 0, length) for axis, length in enumerate(values.shape)]
    longest = values.shape.index(max(values.shape))
    next_to = spot[:longest] + [(spot[longest] + 1) % values.shape[longest]] + spot[longest + 1:]
    return values.at[tuple(spot)].set(least).at[tuple(next_to)].set(largest)


def setup_inputs(seed: int = 0) -> dict:
    key_of = jax.random.split(jax.random.key(seed), 4)
    volt = draw_volt(jax.random.fold_in(key_of[3], 71), 0)
    placement = draw_placement(jax.random.fold_in(key_of[3], 71), 0)
    flags = place_ends((jax.random.randint(key_of[2], (ANTENNAS,), 0, 4) < 3).astype(jnp.int32), jax.random.fold_in(key_of[2], 1), 0, 1)
    return dict(volt=volt, placement=placement, flags=flags)


def reference(volt, placement, flags):
    columns = jnp.arange(GRID_COLUMNS, dtype=jnp.int32)
    onehot = (placement[:, None] == columns[None, :]).astype(jnp.float32) * flags[:, None].astype(jnp.float32)
    onehot = onehot.reshape(NROW, GRID_COLUMNS, GRID_COLUMNS)

    def one_sample(step, running):
        sample = lax.dynamic_index_in_dim(volt, step, 1, keepdims=False)
        gridded = sample.reshape(2, NROW, GRID_COLUMNS, CHANNELS)
        sky_cells = jnp.einsum("sxac,xay->sxyc", gridded, onehot, precision=lax.Precision.HIGHEST)
        spectrum = jnp.fft.fft2(sky_cells[0] + 1j * sky_cells[1], axes=(0, 1))
        return running + jnp.sum(jnp.real(spectrum) ** 2 + jnp.imag(spectrum) ** 2, axis=2)

    running = lax.fori_loop(0, TIMES, one_sample, jnp.zeros((NROW, GRID_COLUMNS), jnp.float32))
    return running * (1.0 / (TIMES * CHANNELS * NROW * GRID_COLUMNS))
```

```python
import math

import jax
import jax.numpy as jnp
import numpy as np
from jax import lax
from jax.experimental import pallas as pl
from jax.experimental.pallas import tpu as pltpu
from jax.sharding import PartitionSpec as P

NROW = 64
GRID_COLUMNS = 64
CHANNELS = 512
TIMES = 128
LANES = 128
CHUNKS = 8
AHEAD = 4
MESH = pl.DeviceIdType.MESH
HIGHEST = lax.Precision.HIGHEST


def fourier_matrix():
    ids = np.outer(np.arange(NROW), np.arange(NROW)) % NROW
    turned = ids * (2.0 * math.pi / NROW)
    cos, sin = np.cos(turned), np.sin(turned)
    return np.block([[cos, sin], [-sin, cos]]).astype(np.float32)


def grid_peer(me, j):
    z_rank = j // 8
    half = (z_rank + 1) // 2
    dz = 4 + half * (1 - 2 * (z_rank % 2))
    dc = 1 - (j // 4) % 2
    dx = 3 - j % 4
    x, z, c = me // 16, (me // 2) % 8, me % 2
    return ((x + dx) % 4) * 16 + ((z + dz) % 8) * 2 + (c + dc) % 2


def kernel(
    volt, placement, flags, table, out,
    staged, rows, cols, table_here, mix, power, parts,
    load_sem, table_sem, send_sem, recv_sem, part_send, part_recv,
):
    me = lax.axis_index("grid")
    group = lax.axis_index("chan")
    grid_count = NROW
    chan_count = parts.shape[0] + 1
    times = staged.shape[2]
    share = out.shape[0]

    loads = [
        pltpu.make_async_copy(volt.at[:, pl.ds(k * times, times)], staged.at[k], load_sem.at[k])
        for k in range(CHUNKS)
    ]
    table_load = pltpu.make_async_copy(table, table_here, table_sem)
    table_load.start()
    for load in loads:
        load.start()

    barrier = pltpu.get_barrier_semaphore()

    def greet(j, carry):
        pl.semaphore_signal(barrier, inc=1, device_id={"grid": grid_peer(me, j)}, device_id_type=MESH)
        return carry

    lax.fori_loop(0, grid_count - 1, greet, 0)
    for d in range(1, chan_count):
        pl.semaphore_signal(
            barrier, inc=1, device_id={"chan": lax.rem(group + d, chan_count)}, device_id_type=MESH
        )

    position = lax.broadcasted_iota(jnp.int32, (GRID_COLUMNS, GRID_COLUMNS), 0)
    pick = jnp.where(position == placement[...], flags[...].astype(jnp.float32), 0.0)
    none = jnp.zeros_like(pick)
    pick = jnp.concatenate(
        [jnp.concatenate([pick, none], axis=1), jnp.concatenate([none, pick], axis=1)], axis=0
    )
    table_load.wait()
    mix[...] = jnp.dot(table_here[...], pick, precision=HIGHEST, preferred_element_type=jnp.float32)
    power[...] = jnp.zeros_like(power)

    def row_dft(k):
        def one_time(t, carry):
            x = staged[k, :, t].reshape(2 * GRID_COLUMNS, LANES)
            y = jnp.dot(mix[...], x, precision=HIGHEST, preferred_element_type=jnp.float32)
            rows[k, 2 * t] = y[:GRID_COLUMNS]
            rows[k, 2 * t + 1] = y[GRID_COLUMNS:]
            return carry

        lax.fori_loop(0, times, one_time, 0)

    def send(k):
        def one_peer(j, carry):
            peer = grid_peer(me, j)
            pltpu.make_async_remote_copy(
                src_ref=rows.at[k, :, peer],
                dst_ref=cols.at[k, :, me],
                send_sem=send_sem.at[k],
                recv_sem=recv_sem.at[k],
                device_id={"grid": peer},
                device_id_type=MESH,
            ).start()
            return carry

        lax.fori_loop(0, grid_count - 1, one_peer, 0)
        cols[k, :, pl.ds(me, 1)] = rows[k, :, pl.ds(me, 1)]

    def all_copies(k):
        return pltpu.make_async_remote_copy(
            src_ref=rows.at[k, :, pl.ds(0, grid_count - 1)],
            dst_ref=cols.at[k, :, pl.ds(0, grid_count - 1)],
            send_sem=send_sem.at[k],
            recv_sem=recv_sem.at[k],
            device_id={"grid": grid_peer(me, 0)},
            device_id_type=MESH,
        )

    def col_dft(k):
        def one_time(t, total):
            x = cols[k, pl.ds(2 * t, 2)].reshape(2 * NROW, LANES)
            y = jnp.dot(table_here[...], x, precision=HIGHEST, preferred_element_type=jnp.float32)
            return total + y * y

        power[...] += lax.fori_loop(0, times, one_time, jnp.zeros((2 * NROW, LANES), jnp.float32))

    loads[0].wait()
    row_dft(0)
    pl.semaphore_wait(barrier, grid_count - 1 + chan_count - 1)
    send(0)
    for k in range(1, AHEAD):
        loads[k].wait()
        row_dft(k)
        send(k)

    for k in range(CHUNKS):
        if k + AHEAD < CHUNKS:
            loads[k + AHEAD].wait()
            row_dft(k + AHEAD)
            send(k + AHEAD)
        all_copies(k).wait_recv()
        col_dft(k)

    power[:NROW] = power[:NROW] + power[NROW:]
    copies = []
    for d in range(1, chan_count):
        peer = lax.rem(group + d, chan_count)
        copies.append(
            pltpu.make_async_remote_copy(
                src_ref=power.at[pl.ds(pl.multiple_of(peer * share, share), share)],
                dst_ref=parts.at[d - 1],
                send_sem=part_send.at[d - 1],
                recv_sem=part_recv.at[d - 1],
                device_id={"chan": peer},
                device_id_type=MESH,
            )
        )
        copies[-1].start()
    for k in range(CHUNKS):
        all_copies(k).wait_send()
    total = power[pl.ds(pl.multiple_of(group * share, share), share)]
    for d in range(1, chan_count):
        copies[d - 1].wait()
        total = total + parts[d - 1]
    out[...] = jnp.sum(total, axis=1, keepdims=True) * (1.0 / (TIMES * CHANNELS * NROW * GRID_COLUMNS))


def on_device(volt, placement, flags):
    times = volt.shape[1] // CHUNKS
    chan_count = lax.axis_size("chan")
    share = NROW // chan_count
    any_space = pl.BlockSpec(memory_space=pl.ANY)
    vmem = pl.BlockSpec(memory_space=pltpu.VMEM)
    return pl.pallas_call(
        kernel,
        name="sky",
        out_shape=jax.ShapeDtypeStruct((share, 1), jnp.float32),
        in_specs=[any_space, vmem, vmem, any_space],
        out_specs=vmem,
        scratch_shapes=[
            pltpu.VMEM((CHUNKS, 2, times, GRID_COLUMNS, LANES), jnp.float32),
            pltpu.VMEM((CHUNKS, 2 * times, GRID_COLUMNS, LANES), jnp.float32),
            pltpu.VMEM((CHUNKS, 2 * times, NROW, LANES), jnp.float32),
            pltpu.VMEM((2 * NROW, 2 * NROW), jnp.float32),
            pltpu.VMEM((2 * GRID_COLUMNS, 2 * GRID_COLUMNS), jnp.float32),
            pltpu.VMEM((2 * NROW, LANES), jnp.float32),
            pltpu.VMEM((chan_count - 1, share, LANES), jnp.float32),
            pltpu.SemaphoreType.DMA((CHUNKS,)),
            pltpu.SemaphoreType.DMA,
            pltpu.SemaphoreType.DMA((CHUNKS,)),
            pltpu.SemaphoreType.DMA((CHUNKS,)),
            pltpu.SemaphoreType.DMA((chan_count - 1,)),
            pltpu.SemaphoreType.DMA((chan_count - 1,)),
        ],
        compiler_params=pltpu.CompilerParams(
            collective_id=0, has_side_effects=True, vmem_limit_bytes=60 * 2**20
        ),
    )(
        volt,
        placement.reshape(1, GRID_COLUMNS),
        flags.reshape(1, GRID_COLUMNS),
        jnp.asarray(fourier_matrix()),
    )


def solution(mesh):
    return jax.shard_map(
        on_device,
        mesh=mesh,
        in_specs=(P(None, None, "grid", "chan"), P("grid"), P("grid")),
        out_specs=P("chan", "grid"),
        check_vma=False,
    )
```

```python
import math

import jax
import jax.numpy as jnp
import numpy as np
from jax import lax
from jax.experimental import pallas as pl
from jax.experimental.pallas import tpu as pltpu
from jax.sharding import PartitionSpec as P

NROW = 64
GRID_COLUMNS = 64
CHANNELS = 512
TIMES = 128
LANES = 128
SIZES = (8, 8, 16, 16, 16, 16, 16, 16, 8, 4, 4)
STARTS = tuple(sum(SIZES[:k]) for k in range(len(SIZES)))
AHEAD = 64
UNROLL = 8
MESH = pl.DeviceIdType.MESH
HIGHEST = lax.Precision.HIGHEST


def fourier_matrix():
    ids = np.outer(np.arange(NROW), np.arange(NROW)) % NROW
    turned = ids * (2.0 * math.pi / NROW)
    cos, sin = np.cos(turned), np.sin(turned)
    return np.block([[cos, sin], [-sin, cos]]).astype(np.float32)


def z_ring_peer(me, j):
    rank = j // 2
    half = (rank + 1) // 2
    dz = 4 + half * (1 - 2 * (rank % 2))
    dc = 1 - j % 2
    x, z, c = me // 16, (me // 2) % 8, me % 2
    return x * 16 + ((z + dz) % 8) * 2 + (c + dc) % 2


def other_peer(me, j):
    rank = j // 6
    half = (rank + 1) // 2
    dz = 4 + half * (1 - 2 * (rank % 2))
    dc = 1 - (j // 3) % 2
    dx = 3 - j % 3
    x, z, c = me // 16, (me // 2) % 8, me % 2
    return ((x + dx) % 4) * 16 + ((z + dz) % 8) * 2 + (c + dc) % 2


def line_peer(me, d):
    return (me + 16 * d) % 64


def kernel(
    volt, placement, flags, table, out,
    staged, rows, cols, table_here, placement_here, flags_here, mix, power, parts,
    load_sem, small_sem, send_sem, recv_sem, ring_sem, part_send, part_recv,
):
    me = lax.axis_index("grid")
    group = lax.axis_index("chan")
    chan_count = parts.shape[0] + 1
    share = parts.shape[1]
    chunks = len(SIZES)

    def signal(semaphore, peer):
        pl.semaphore_signal(semaphore, inc=1, device_id=peer, device_id_type=MESH)

    barrier = pltpu.get_barrier_semaphore()
    for j in range(15):
        signal(barrier, {"grid": z_ring_peer(me, j)})
    for d in (2, 1, 3):
        signal(barrier, {"grid": line_peer(me, d)})
    for d in range(1, chan_count):
        signal(barrier, {"chan": lax.rem(group + d, chan_count)})

    loads = [
        pltpu.make_async_copy(
            volt.at[:, pl.ds(STARTS[k], SIZES[k])], staged.at[:, pl.ds(STARTS[k], SIZES[k])], load_sem.at[k]
        )
        for k in range(chunks)
    ]
    small = [
        pltpu.make_async_copy(placement, placement_here, small_sem.at[0]),
        pltpu.make_async_copy(flags, flags_here, small_sem.at[1]),
        pltpu.make_async_copy(table, table_here, small_sem.at[2]),
    ]
    for load in small + loads[:2]:
        load.start()
    for load in small:
        load.wait()

    position = lax.broadcasted_iota(jnp.int32, (GRID_COLUMNS, GRID_COLUMNS), 0)
    pick = jnp.where(position == placement_here[...], flags_here[...].astype(jnp.float32), 0.0)
    none = jnp.zeros_like(pick)
    pick = jnp.concatenate(
        [jnp.concatenate([pick, none], axis=1), jnp.concatenate([none, pick], axis=1)], axis=0
    )
    mix[...] = jnp.dot(table_here[...], pick, precision=HIGHEST, preferred_element_type=jnp.float32)
    power[...] = jnp.zeros_like(power)

    def row_dft(k):
        def one_time(i, carry):
            t = STARTS[k] + i
            x = staged[:, t].reshape(2 * GRID_COLUMNS, LANES)
            y = jnp.dot(mix[...], x, precision=HIGHEST, preferred_element_type=jnp.float32)
            rows[2 * t] = y[:GRID_COLUMNS]
            rows[2 * t + 1] = y[GRID_COLUMNS:]
            return carry

        lax.fori_loop(0, SIZES[k], one_time, 0)

    def span(k):
        return pl.ds(2 * STARTS[k], 2 * SIZES[k])

    def send_to(k, peer):
        pltpu.make_async_remote_copy(
            src_ref=rows.at[span(k), peer],
            dst_ref=cols.at[span(k), me],
            send_sem=send_sem.at[k],
            recv_sem=recv_sem.at[k],
            device_id={"grid": peer},
            device_id_type=MESH,
        ).start()

    def send_ring(k):
        def one_peer(j, carry):
            send_to(k, z_ring_peer(me, j))
            return carry

        lax.fori_loop(0, 15, one_peer, 0, unroll=UNROLL)

    def send_others(k):
        def one_peer(j, carry):
            send_to(k, other_peer(me, j))
            return carry

        lax.fori_loop(0, 48, one_peer, 0, unroll=UNROLL)
        cols[span(k), pl.ds(me, 1)] = rows[span(k), pl.ds(me, 1)]

    def all_copies(k):
        return pltpu.make_async_remote_copy(
            src_ref=rows.at[span(k), pl.ds(0, NROW - 1)],
            dst_ref=cols.at[span(k), pl.ds(0, NROW - 1)],
            send_sem=send_sem.at[k],
            recv_sem=recv_sem.at[k],
            device_id={"grid": line_peer(me, 1)},
            device_id_type=MESH,
        )

    def col_dft(k):
        all_copies(k).wait_recv()

        def one_time(i, total):
            x = cols[pl.ds(2 * (STARTS[k] + i), 2)].reshape(2 * NROW, LANES)
            y = jnp.dot(table_here[...], x, precision=HIGHEST, preferred_element_type=jnp.float32)
            return total + y * y

        power[...] += lax.fori_loop(0, SIZES[k], one_time, jnp.zeros((2 * NROW, LANES), jnp.float32))

    loads[0].wait()
    for load in loads[2:]:
        load.start()
    row_dft(0)
    pl.semaphore_wait(barrier, 15 + 3 + chan_count - 1)
    for d in (2, 1, 3):
        signal(ring_sem, {"grid": line_peer(me, d)})
    send_ring(0)
    pl.semaphore_wait(ring_sem, 3)
    send_others(0)

    received = 0
    for k in range(1, chunks):
        while STARTS[k] - STARTS[received] >= AHEAD:
            col_dft(received)
            received += 1
        loads[k].wait()
        row_dft(k)
        send_ring(k)
        send_others(k)
    for k in range(received, chunks):
        col_dft(k)

    power[:NROW] = power[:NROW] + power[NROW:]
    copies = []
    for d in (2, 1, 3):
        peer = lax.rem(group + d, chan_count)
        copies.append(
            pltpu.make_async_remote_copy(
                src_ref=power.at[pl.ds(pl.multiple_of(peer * share, share), share)],
                dst_ref=parts.at[d - 1],
                send_sem=part_send.at[d - 1],
                recv_sem=part_recv.at[d - 1],
                device_id={"chan": peer},
                device_id_type=MESH,
            )
        )
        copies[-1].start()
    for k in range(chunks):
        all_copies(k).wait_send()
    for copy in copies:
        copy.wait()
    total = power[pl.ds(pl.multiple_of(group * share, share), share)]
    total = (total + parts[0]) + (parts[1] + parts[2])
    out[...] = jnp.sum(total.T, axis=0, keepdims=True) * (1.0 / (TIMES * CHANNELS * NROW * GRID_COLUMNS))


def on_device(volt, placement, flags):
    chan_count = lax.axis_size("chan")
    share = NROW // chan_count
    hbm = pl.BlockSpec(memory_space=pltpu.HBM)
    vmem = pl.BlockSpec(memory_space=pltpu.VMEM)
    image = pl.pallas_call(
        kernel,
        name="sky",
        out_shape=pltpu.VMEM((1, share), jnp.float32),
        in_specs=[hbm, hbm, hbm, hbm],
        out_specs=vmem,
        scratch_shapes=[
            pltpu.VMEM((2, TIMES, GRID_COLUMNS, LANES), jnp.float32),
            pltpu.VMEM((2 * TIMES, GRID_COLUMNS, LANES), jnp.float32),
            pltpu.VMEM((2 * TIMES, NROW, LANES), jnp.float32),
            pltpu.VMEM((2 * NROW, 2 * NROW), jnp.float32),
            pltpu.VMEM((1, GRID_COLUMNS), jnp.int32),
            pltpu.VMEM((1, GRID_COLUMNS), jnp.int32),
            pltpu.VMEM((2 * GRID_COLUMNS, 2 * GRID_COLUMNS), jnp.float32),
            pltpu.VMEM((2 * NROW, LANES), jnp.float32),
            pltpu.VMEM((chan_count - 1, share, LANES), jnp.float32),
            pltpu.SemaphoreType.DMA((len(SIZES),)),
            pltpu.SemaphoreType.DMA((3,)),
            pltpu.SemaphoreType.DMA((len(SIZES),)),
            pltpu.SemaphoreType.DMA((len(SIZES),)),
            pltpu.SemaphoreType.REGULAR,
            pltpu.SemaphoreType.DMA((chan_count - 1,)),
            pltpu.SemaphoreType.DMA((chan_count - 1,)),
        ],
        compiler_params=pltpu.CompilerParams(
            collective_id=0, has_side_effects=True, vmem_limit_bytes=60 * 2**20
        ),
    )(
        volt,
        placement.reshape(1, GRID_COLUMNS),
        flags.reshape(1, GRID_COLUMNS),
        jnp.asarray(fourier_matrix()),
    )
    return image.reshape(share, 1)


def solution(mesh):
    return jax.shard_map(
        on_device,
        mesh=mesh,
        in_specs=(P(None, None, "grid", "chan"), P("grid"), P("grid")),
        out_specs=P("chan", "grid"),
        check_vma=False,
    )
```

```python
import math

import jax
import jax.numpy as jnp
import numpy as np
from jax import lax
from jax.experimental import pallas as pl
from jax.experimental.pallas import tpu as pltpu
from jax.sharding import PartitionSpec as P

NROW = 64
GRID_COLUMNS = 64
CHANNELS = 512
TIMES = 128
LANES = 128
SIZES = (8, 8, 16, 16, 16, 16, 16, 16, 8, 4, 2, 2)
STARTS = tuple(sum(SIZES[:k]) for k in range(len(SIZES)))
AHEAD = 64
UNROLL = 8
MESH = pl.DeviceIdType.MESH
HIGHEST = lax.Precision.HIGHEST


def fourier_matrix():
    ids = np.outer(np.arange(NROW), np.arange(NROW)) % NROW
    turned = ids * (2.0 * math.pi / NROW)
    cos, sin = np.cos(turned), np.sin(turned)
    return np.block([[cos, sin], [-sin, cos]]).astype(np.float32)


def at_offset(me, dx, dz, core):
    x, z = me // 16, (me // 2) % 8
    return ((x + dx) % 4) * 16 + ((z + dz) % 8) * 2 + core


def near_peer(me, j):
    rank = j // 2
    return at_offset(me, 0, 2 - rank - rank // 2, j % 2)


def far_peer(me, j):
    return at_offset(me, 0, 3 + j // 2, j % 2)


def core_mate(me):
    return me + 1 - 2 * (me % 2)


def other_peer(me, j):
    rank = j // 6
    half = (rank + 1) // 2
    return at_offset(me, 3 - j % 3, 4 + half * (1 - 2 * (rank % 2)), (j // 3) % 2)


def last_peer(me, j):
    core, rest = j // 31, j % 31
    rank = rest // 4
    half = (rank + 1) // 2
    return at_offset(me, 3 - rest % 4, 4 + half * (1 - 2 * (rank % 2)), core)


def line_peer(me, d):
    return (me + 16 * d) % 64


def kernel(
    volt, placement, flags, table, out,
    staged, rows, cols, table_here, placement_here, flags_here, mix, power, parts,
    load_sem, small_sem, send_sem, recv_sem, near_sem, ring_sem, part_send, part_recv,
):
    me = lax.axis_index("grid")
    group = lax.axis_index("chan")
    chan_count = parts.shape[0] + 1
    share = parts.shape[1]
    chunks = len(SIZES)

    def signal(semaphore, peer):
        pl.semaphore_signal(semaphore, inc=1, device_id=peer, device_id_type=MESH)

    loads = [
        pltpu.make_async_copy(
            volt.at[:, pl.ds(STARTS[k], SIZES[k])], staged.at[:, pl.ds(STARTS[k], SIZES[k])], load_sem.at[k]
        )
        for k in range(chunks)
    ]
    small = [
        pltpu.make_async_copy(placement, placement_here, small_sem.at[0]),
        pltpu.make_async_copy(flags, flags_here, small_sem.at[1]),
        pltpu.make_async_copy(table, table_here, small_sem.at[2]),
    ]
    for load in small:
        load.start()

    barrier = pltpu.get_barrier_semaphore()
    for j in range(8):
        signal(barrier, {"grid": near_peer(me, j)})
    for d in (2, 1, 3):
        signal(barrier, {"grid": line_peer(me, d)})
        signal(barrier, {"chan": lax.rem(group + d, chan_count)})
    signal(barrier, {"grid": core_mate(me)})

    for load in loads[:2]:
        load.start()
    for load in small:
        load.wait()

    position = lax.broadcasted_iota(jnp.int32, (GRID_COLUMNS, GRID_COLUMNS), 0)
    pick = jnp.where(position == placement_here[...], flags_here[...].astype(jnp.float32), 0.0)
    none = jnp.zeros_like(pick)
    pick = jnp.concatenate(
        [jnp.concatenate([pick, none], axis=1), jnp.concatenate([none, pick], axis=1)], axis=0
    )
    mix[...] = jnp.dot(table_here[...], pick, precision=HIGHEST, preferred_element_type=jnp.float32)
    power[...] = jnp.zeros_like(power)

    def row_dft(k):
        def one_time(i, carry):
            t = STARTS[k] + i
            x = staged[:, t].reshape(2 * GRID_COLUMNS, LANES)
            y = jnp.dot(mix[...], x, precision=HIGHEST, preferred_element_type=jnp.float32)
            rows[2 * t] = y[:GRID_COLUMNS]
            rows[2 * t + 1] = y[GRID_COLUMNS:]
            return carry

        lax.fori_loop(0, SIZES[k], one_time, 0)

    def span(k):
        return pl.ds(2 * STARTS[k], 2 * SIZES[k])

    def send_to(k, peer):
        pltpu.make_async_remote_copy(
            src_ref=rows.at[span(k), peer],
            dst_ref=cols.at[span(k), me],
            send_sem=send_sem.at[k],
            recv_sem=recv_sem.at[k],
            device_id={"grid": peer},
            device_id_type=MESH,
        ).start()

    def send_all(k, count, peer_at):
        def one_peer(j, carry):
            send_to(k, peer_at(me, j))
            return carry

        lax.fori_loop(0, count, one_peer, 0, unroll=UNROLL)

    def send_chunk(k):
        if k < chunks - 1:
            send_all(k, 6, far_peer)
            send_all(k, 48, other_peer)
            send_all(k, 8, near_peer)
        else:
            send_all(k, 62, last_peer)
        send_to(k, core_mate(me))
        keep_own(k)

    def keep_own(k):
        cols[span(k), pl.ds(me, 1)] = rows[span(k), pl.ds(me, 1)]

    def all_copies(k):
        return pltpu.make_async_remote_copy(
            src_ref=rows.at[span(k), pl.ds(0, NROW - 1)],
            dst_ref=cols.at[span(k), pl.ds(0, NROW - 1)],
            send_sem=send_sem.at[k],
            recv_sem=recv_sem.at[k],
            device_id={"grid": line_peer(me, 1)},
            device_id_type=MESH,
        )

    def col_dft(k):
        all_copies(k).wait_recv()

        def one_time(i, total):
            x = cols[pl.ds(2 * (STARTS[k] + i), 2)].reshape(2 * NROW, LANES)
            y = jnp.dot(table_here[...], x, precision=HIGHEST, preferred_element_type=jnp.float32)
            return total + y * y

        power[...] += lax.fori_loop(0, SIZES[k], one_time, jnp.zeros((2 * NROW, LANES), jnp.float32))

    loads[0].wait()
    for load in loads[2:]:
        load.start()
    row_dft(0)
    pl.semaphore_wait(barrier, 8 + 3 + chan_count - 1 + 1)
    for dz in (2, 6, 1, 7):
        signal(near_sem, {"grid": at_offset(me, 0, dz, me % 2)})
    send_all(0, 8, near_peer)
    send_to(0, core_mate(me))
    pl.semaphore_wait(near_sem, 4)
    for d in (2, 1, 3):
        signal(ring_sem, {"grid": line_peer(me, d)})
    send_all(0, 6, far_peer)
    keep_own(0)
    pl.semaphore_wait(ring_sem, 3)
    send_all(0, 48, other_peer)

    received = 0
    for k in range(1, chunks):
        while STARTS[k] - STARTS[received] >= AHEAD:
            col_dft(received)
            received += 1
        loads[k].wait()
        row_dft(k)
        send_chunk(k)
    for k in range(received, chunks):
        col_dft(k)

    power[:NROW] = power[:NROW] + power[NROW:]
    copies = []
    for d in (2, 1, 3):
        peer = lax.rem(group + d, chan_count)
        copies.append(
            pltpu.make_async_remote_copy(
                src_ref=power.at[pl.ds(pl.multiple_of(peer * share, share), share)],
                dst_ref=parts.at[d - 1],
                send_sem=part_send.at[d - 1],
                recv_sem=part_recv.at[d - 1],
                device_id={"chan": peer},
                device_id_type=MESH,
            )
        )
        copies[-1].start()
    for k in range(chunks):
        all_copies(k).wait_send()
    for copy in copies:
        copy.wait()
    total = power[pl.ds(pl.multiple_of(group * share, share), share)]
    total = (total + parts[0]) + (parts[1] + parts[2])
    out[...] = jnp.sum(total.T, axis=0, keepdims=True) * (1.0 / (TIMES * CHANNELS * NROW * GRID_COLUMNS))


def on_device(volt, placement, flags):
    chan_count = lax.axis_size("chan")
    share = NROW // chan_count
    hbm = pl.BlockSpec(memory_space=pltpu.HBM)
    vmem = pl.BlockSpec(memory_space=pltpu.VMEM)
    image = pl.pallas_call(
        kernel,
        name="sky",
        out_shape=pltpu.VMEM((1, share), jnp.float32),
        in_specs=[hbm, hbm, hbm, hbm],
        out_specs=vmem,
        scratch_shapes=[
            pltpu.VMEM((2, TIMES, GRID_COLUMNS, LANES), jnp.float32),
            pltpu.VMEM((2 * TIMES, GRID_COLUMNS, LANES), jnp.float32),
            pltpu.VMEM((2 * TIMES, NROW, LANES), jnp.float32),
            pltpu.VMEM((2 * NROW, 2 * NROW), jnp.float32),
            pltpu.VMEM((1, GRID_COLUMNS), jnp.int32),
            pltpu.VMEM((1, GRID_COLUMNS), jnp.int32),
            pltpu.VMEM((2 * GRID_COLUMNS, 2 * GRID_COLUMNS), jnp.float32),
            pltpu.VMEM((2 * NROW, LANES), jnp.float32),
            pltpu.VMEM((chan_count - 1, share, LANES), jnp.float32),
            pltpu.SemaphoreType.DMA((len(SIZES),)),
            pltpu.SemaphoreType.DMA((3,)),
            pltpu.SemaphoreType.DMA((len(SIZES),)),
            pltpu.SemaphoreType.DMA((len(SIZES),)),
            pltpu.SemaphoreType.REGULAR,
            pltpu.SemaphoreType.REGULAR,
            pltpu.SemaphoreType.DMA((chan_count - 1,)),
            pltpu.SemaphoreType.DMA((chan_count - 1,)),
        ],
        compiler_params=pltpu.CompilerParams(
            collective_id=0, has_side_effects=True, vmem_limit_bytes=60 * 2**20
        ),
    )(
        volt,
        placement.reshape(1, GRID_COLUMNS),
        flags.reshape(1, GRID_COLUMNS),
        jnp.asarray(fourier_matrix()),
    )
    return image.reshape(share, 1)


def solution(mesh):
    return jax.shard_map(
        on_device,
        mesh=mesh,
        in_specs=(P(None, None, "grid", "chan"), P("grid"), P("grid")),
        out_specs=P("chan", "grid"),
        check_vma=False,
    )
```

```python
import math

import jax
import jax.numpy as jnp
import numpy as np
from jax import lax
from jax.experimental import pallas as pl
from jax.experimental.pallas import tpu as pltpu
from jax.sharding import PartitionSpec as P

NROW = 64
GRID_COLUMNS = 64
CHANNELS = 512
TIMES = 128
LANES = 128
SIZES = (8, 8, 16, 16, 16, 16, 16, 16, 8, 4, 2, 2)
STARTS = tuple(sum(SIZES[:k]) for k in range(len(SIZES)))
AHEAD = 64
UNROLL = 8
MESH = pl.DeviceIdType.MESH
HIGHEST = lax.Precision.HIGHEST


def fourier_matrix():
    ids = np.outer(np.arange(NROW), np.arange(NROW)) % NROW
    turned = ids * (2.0 * math.pi / NROW)
    cos, sin = np.cos(turned), np.sin(turned)
    return np.block([[cos, sin], [-sin, cos]]).astype(np.float32)


def at_offset(me, dx, dz, core):
    x, z = me // 16, (me // 2) % 8
    return ((x + dx) % 4) * 16 + ((z + dz) % 8) * 2 + core


def near_peer(me, j):
    rank = j // 2
    return at_offset(me, 0, 2 - rank - rank // 2, j % 2)


def far_peer(me, j):
    return at_offset(me, 0, 3 + j // 2, j % 2)


def core_mate(me):
    return me + 1 - 2 * (me % 2)


def other_peer(me, j):
    rank = j // 6
    half = (rank + 1) // 2
    return at_offset(me, 3 - j % 3, 4 + half * (1 - 2 * (rank % 2)), (j // 3) % 2)


def last_peer(me, j):
    core, rest = j // 31, j % 31
    rank = rest // 4
    half = (rank + 1) // 2
    return at_offset(me, 3 - rest % 4, 4 + half * (1 - 2 * (rank % 2)), core)


def line_peer(me, d):
    return (me + 16 * d) % 64


def kernel(
    volt, placement, flags, table, out,
    staged, rows, cols, table_here, placement_here, flags_here, mix, power, parts,
    load_sem, small_sem, send_sem, recv_sem, near_sem, ring_sem, part_send, part_recv,
):
    me = lax.axis_index("grid")
    group = lax.axis_index("chan")
    chan_count = parts.shape[0] + 1
    share = parts.shape[1]
    chunks = len(SIZES)

    def signal(semaphore, peer):
        pl.semaphore_signal(semaphore, inc=1, device_id=peer, device_id_type=MESH)

    loads = [
        pltpu.make_async_copy(
            volt.at[:, pl.ds(STARTS[k], SIZES[k])], staged.at[:, pl.ds(STARTS[k], SIZES[k])], load_sem.at[k]
        )
        for k in range(chunks)
    ]
    small = [
        pltpu.make_async_copy(placement, placement_here, small_sem.at[0]),
        pltpu.make_async_copy(flags, flags_here, small_sem.at[1]),
        pltpu.make_async_copy(table, table_here, small_sem.at[2]),
    ]
    for load in small:
        load.start()

    barrier = pltpu.get_barrier_semaphore()
    for j in range(8):
        signal(barrier, {"grid": near_peer(me, j)})
    for d in (2, 1, 3):
        signal(barrier, {"grid": line_peer(me, d)})
        signal(barrier, {"chan": lax.rem(group + d, chan_count)})
    signal(barrier, {"grid": core_mate(me)})

    for load in loads[:2]:
        load.start()
    for load in small:
        load.wait()

    position = lax.broadcasted_iota(jnp.int32, (GRID_COLUMNS, GRID_COLUMNS), 0)
    pick = jnp.where(position == placement_here[...], flags_here[...].astype(jnp.float32), 0.0)
    none = jnp.zeros_like(pick)
    pick = jnp.concatenate(
        [jnp.concatenate([pick, none], axis=1), jnp.concatenate([none, pick], axis=1)], axis=0
    )
    mix[...] = jnp.dot(table_here[...], pick, precision=HIGHEST, preferred_element_type=jnp.float32)
    power[...] = jnp.zeros_like(power)

    def row_dft(k):
        def one_time(i, carry):
            t = STARTS[k] + i
            x = staged[:, t].reshape(2 * GRID_COLUMNS, LANES)
            y = jnp.dot(mix[...], x, precision=HIGHEST, preferred_element_type=jnp.float32)
            rows[2 * t] = y[:GRID_COLUMNS]
            rows[2 * t + 1] = y[GRID_COLUMNS:]
            return carry

        lax.fori_loop(0, SIZES[k], one_time, 0)

    def span(k):
        return pl.ds(2 * STARTS[k], 2 * SIZES[k])

    def send_to(k, peer):
        pltpu.make_async_remote_copy(
            src_ref=rows.at[span(k), peer],
            dst_ref=cols.at[span(k), me],
            send_sem=send_sem.at[k],
            recv_sem=recv_sem.at[k],
            device_id={"grid": peer},
            device_id_type=MESH,
        ).start()

    def send_all(k, count, peer_at):
        def one_peer(j, carry):
            send_to(k, peer_at(me, j))
            return carry

        lax.fori_loop(0, count, one_peer, 0, unroll=UNROLL)

    def send_near(k):
        send_all(k, 8, near_peer)
        send_to(k, core_mate(me))

    def send_chunk(k):
        if k < chunks - 1:
            send_all(k, 6, far_peer)
            send_near(k)
            send_all(k, 48, other_peer)
        else:
            send_all(k, 62, last_peer)
            send_to(k, core_mate(me))
        keep_own(k)

    def keep_own(k):
        cols[span(k), pl.ds(me, 1)] = rows[span(k), pl.ds(me, 1)]

    def all_copies(k):
        return pltpu.make_async_remote_copy(
            src_ref=rows.at[span(k), pl.ds(0, NROW - 1)],
            dst_ref=cols.at[span(k), pl.ds(0, NROW - 1)],
            send_sem=send_sem.at[k],
            recv_sem=recv_sem.at[k],
            device_id={"grid": line_peer(me, 1)},
            device_id_type=MESH,
        )

    def col_dft(k):
        all_copies(k).wait_recv()

        def one_time(i, total):
            x = cols[pl.ds(2 * (STARTS[k] + i), 2)].reshape(2 * NROW, LANES)
            y = jnp.dot(table_here[...], x, precision=HIGHEST, preferred_element_type=jnp.float32)
            return total + y * y

        power[...] += lax.fori_loop(0, SIZES[k], one_time, jnp.zeros((2 * NROW, LANES), jnp.float32))

    loads[0].wait()
    for load in loads[2:]:
        load.start()
    row_dft(0)
    pl.semaphore_wait(barrier, 8 + 3 + chan_count - 1 + 1)
    for dz in (2, 6, 1, 7):
        signal(near_sem, {"grid": at_offset(me, 0, dz, me % 2)})
    send_near(0)
    loads[1].wait()
    row_dft(1)
    send_near(1)
    pl.semaphore_wait(near_sem, 4)
    for d in (2, 1, 3):
        signal(ring_sem, {"grid": line_peer(me, d)})
    for k in (0, 1):
        send_all(k, 6, far_peer)
    for k in (0, 1):
        keep_own(k)
    pl.semaphore_wait(ring_sem, 3)
    for k in (0, 1):
        send_all(k, 48, other_peer)

    received = 0
    for k in range(2, chunks):
        while STARTS[k] - STARTS[received] >= AHEAD:
            col_dft(received)
            received += 1
        loads[k].wait()
        row_dft(k)
        send_chunk(k)
    for k in range(received, chunks):
        col_dft(k)

    power[:NROW] = power[:NROW] + power[NROW:]
    copies = []
    for d in (2, 1, 3):
        peer = lax.rem(group + d, chan_count)
        copies.append(
            pltpu.make_async_remote_copy(
                src_ref=power.at[pl.ds(pl.multiple_of(peer * share, share), share)],
                dst_ref=parts.at[d - 1],
                send_sem=part_send.at[d - 1],
                recv_sem=part_recv.at[d - 1],
                device_id={"chan": peer},
                device_id_type=MESH,
            )
        )
        copies[-1].start()
    for k in range(chunks):
        all_copies(k).wait_send()
    for copy in copies:
        copy.wait()
    total = power[pl.ds(pl.multiple_of(group * share, share), share)]
    total = (total + parts[0]) + (parts[1] + parts[2])
    out[...] = jnp.sum(total.T, axis=0, keepdims=True) * (1.0 / (TIMES * CHANNELS * NROW * GRID_COLUMNS))


def on_device(volt, placement, flags):
    chan_count = lax.axis_size("chan")
    share = NROW // chan_count
    hbm = pl.BlockSpec(memory_space=pltpu.HBM)
    vmem = pl.BlockSpec(memory_space=pltpu.VMEM)
    image = pl.pallas_call(
        kernel,
        name="sky",
        out_shape=pltpu.VMEM((1, share), jnp.float32),
        in_specs=[hbm, hbm, hbm, hbm],
        out_specs=vmem,
        scratch_shapes=[
            pltpu.VMEM((2, TIMES, GRID_COLUMNS, LANES), jnp.float32),
            pltpu.VMEM((2 * TIMES, GRID_COLUMNS, LANES), jnp.float32),
            pltpu.VMEM((2 * TIMES, NROW, LANES), jnp.float32),
            pltpu.VMEM((2 * NROW, 2 * NROW), jnp.float32),
            pltpu.VMEM((1, GRID_COLUMNS), jnp.int32),
            pltpu.VMEM((1, GRID_COLUMNS), jnp.int32),
            pltpu.VMEM((2 * GRID_COLUMNS, 2 * GRID_COLUMNS), jnp.float32),
            pltpu.VMEM((2 * NROW, LANES), jnp.float32),
            pltpu.VMEM((chan_count - 1, share, LANES), jnp.float32),
            pltpu.SemaphoreType.DMA((len(SIZES),)),
            pltpu.SemaphoreType.DMA((3,)),
            pltpu.SemaphoreType.DMA((len(SIZES),)),
            pltpu.SemaphoreType.DMA((len(SIZES),)),
            pltpu.SemaphoreType.REGULAR,
            pltpu.SemaphoreType.REGULAR,
            pltpu.SemaphoreType.DMA((chan_count - 1,)),
            pltpu.SemaphoreType.DMA((chan_count - 1,)),
        ],
        compiler_params=pltpu.CompilerParams(
            collective_id=0, has_side_effects=True, vmem_limit_bytes=60 * 2**20
        ),
    )(
        volt,
        placement.reshape(1, GRID_COLUMNS),
        flags.reshape(1, GRID_COLUMNS),
        jnp.asarray(fourier_matrix()),
    )
    return image.reshape(share, 1)


def solution(mesh):
    return jax.shard_map(
        on_device,
        mesh=mesh,
        in_specs=(P(None, None, "grid", "chan"), P("grid"), P("grid")),
        out_specs=P("chan", "grid"),
        check_vma=False,
    )
```

```python
import math

import jax
import jax.numpy as jnp
import numpy as np
from jax import lax
from jax.experimental import pallas as pl
from jax.experimental.pallas import tpu as pltpu
from jax.sharding import PartitionSpec as P

NROW = 64
GRID_COLUMNS = 64
CHANNELS = 512
TIMES = 128
LANES = 128
SIZES = (8, 8, 16, 16, 16, 16, 16, 16, 8, 4, 2, 2)
STARTS = tuple(sum(SIZES[:k]) for k in range(len(SIZES)))
AHEAD = 64
TAIL = 3
UNROLL = 8
MESH = pl.DeviceIdType.MESH
HIGHEST = lax.Precision.HIGHEST


def fourier_matrix():
    ids = np.outer(np.arange(NROW), np.arange(NROW)) % NROW
    turned = ids * (2.0 * math.pi / NROW)
    cos, sin = np.cos(turned), np.sin(turned)
    return np.block([[cos, sin], [-sin, cos]]).astype(np.float32)


def at_offset(me, dx, dz, core):
    x, z = me // 16, (me // 2) % 8
    return ((x + dx) % 4) * 16 + ((z + dz) % 8) * 2 + core


def near_peer(me, j):
    rank = j // 2
    return at_offset(me, 0, 2 - rank - rank // 2, j % 2)


def far_peer(me, j):
    return at_offset(me, 0, 3 + j // 2, j % 2)


def core_mate(me):
    return me + 1 - 2 * (me % 2)


def other_peer(me, j):
    rank = j // 6
    half = (rank + 1) // 2
    return at_offset(me, 3 - j % 3, 4 + half * (1 - 2 * (rank % 2)), (j // 3) % 2)


def tail_far_peer(me, j):
    rank = j // 8
    return at_offset(me, 3 - j % 4, 4 + (rank + 1) // 2 * (1 - 2 * (rank % 2)), (j // 4) % 2)


def tail_near_peer(me, j, core):
    rank = j // 4
    return at_offset(me, 3 - j % 4, (2 - rank // 2) * (1 - 2 * (rank % 2)), core)


def line_peer(me, d):
    return (me + 16 * d) % 64


def kernel(
    volt, placement, flags, table, out,
    staged, rows, cols, table_here, placement_here, flags_here, mix, power, parts,
    load_sem, small_sem, send_sem, recv_sem, near_sem, ring_sem, part_send, part_recv,
):
    me = lax.axis_index("grid")
    group = lax.axis_index("chan")
    chan_count = parts.shape[0] + 1
    share = parts.shape[1]
    chunks = len(SIZES)

    def signal(semaphore, peer):
        pl.semaphore_signal(semaphore, inc=1, device_id=peer, device_id_type=MESH)

    loads = [
        pltpu.make_async_copy(
            volt.at[:, pl.ds(STARTS[k], SIZES[k])], staged.at[:, pl.ds(STARTS[k], SIZES[k])], load_sem.at[k]
        )
        for k in range(chunks)
    ]
    small = [
        pltpu.make_async_copy(placement, placement_here, small_sem.at[0]),
        pltpu.make_async_copy(flags, flags_here, small_sem.at[1]),
        pltpu.make_async_copy(table, table_here, small_sem.at[2]),
    ]
    for load in small:
        load.start()

    barrier = pltpu.get_barrier_semaphore()
    for j in range(8):
        signal(barrier, {"grid": near_peer(me, j)})
    for d in (2, 1, 3):
        signal(barrier, {"grid": line_peer(me, d)})
        signal(barrier, {"chan": lax.rem(group + d, chan_count)})
    signal(barrier, {"grid": core_mate(me)})

    for load in loads[:2]:
        load.start()
    for load in small:
        load.wait()

    position = lax.broadcasted_iota(jnp.int32, (GRID_COLUMNS, GRID_COLUMNS), 0)
    pick = jnp.where(position == placement_here[...], flags_here[...].astype(jnp.float32), 0.0)
    none = jnp.zeros_like(pick)
    pick = jnp.concatenate(
        [jnp.concatenate([pick, none], axis=1), jnp.concatenate([none, pick], axis=1)], axis=0
    )
    mix[...] = jnp.dot(table_here[...], pick, precision=HIGHEST, preferred_element_type=jnp.float32)
    power[...] = jnp.zeros_like(power)

    def row_dft(k):
        def one_time(i, carry):
            t = STARTS[k] + i
            x = staged[:, t].reshape(2 * GRID_COLUMNS, LANES)
            y = jnp.dot(mix[...], x, precision=HIGHEST, preferred_element_type=jnp.float32)
            rows[2 * t] = y[:GRID_COLUMNS]
            rows[2 * t + 1] = y[GRID_COLUMNS:]
            return carry

        lax.fori_loop(0, SIZES[k], one_time, 0)

    def span(k):
        return pl.ds(2 * STARTS[k], 2 * SIZES[k])

    def send_to(k, peer):
        pltpu.make_async_remote_copy(
            src_ref=rows.at[span(k), peer],
            dst_ref=cols.at[span(k), me],
            send_sem=send_sem.at[k],
            recv_sem=recv_sem.at[k],
            device_id={"grid": peer},
            device_id_type=MESH,
        ).start()

    def send_all(k, count, peer_at):
        def one_peer(j, carry):
            send_to(k, peer_at(me, j))
            return carry

        lax.fori_loop(0, count, one_peer, 0, unroll=UNROLL)

    def send_near(k):
        send_all(k, 8, near_peer)
        send_to(k, core_mate(me))

    def send_chunk(k):
        send_all(k, 6, far_peer)
        send_near(k)
        send_all(k, 48, other_peer)
        keep_own(k)

    def send_tail(ks):
        for k in ks:
            send_all(k, 24, tail_far_peer)
        for k in ks:
            send_to(k, core_mate(me))
            keep_own(k)
        for core in (0, 1):
            for k in ks:
                send_all(k, 19, lambda me, j: tail_near_peer(me, j, core))

    def keep_own(k):
        cols[span(k), pl.ds(me, 1)] = rows[span(k), pl.ds(me, 1)]

    def all_copies(k):
        return pltpu.make_async_remote_copy(
            src_ref=rows.at[span(k), pl.ds(0, NROW - 1)],
            dst_ref=cols.at[span(k), pl.ds(0, NROW - 1)],
            send_sem=send_sem.at[k],
            recv_sem=recv_sem.at[k],
            device_id={"grid": line_peer(me, 1)},
            device_id_type=MESH,
        )

    def col_dft(k):
        all_copies(k).wait_recv()

        def one_time(i, total):
            x = cols[pl.ds(2 * (STARTS[k] + i), 2)].reshape(2 * NROW, LANES)
            y = jnp.dot(table_here[...], x, precision=HIGHEST, preferred_element_type=jnp.float32)
            return total + y * y

        power[...] += lax.fori_loop(0, SIZES[k], one_time, jnp.zeros((2 * NROW, LANES), jnp.float32))

    loads[0].wait()
    for load in loads[2:]:
        load.start()
    row_dft(0)
    pl.semaphore_wait(barrier, 8 + 3 + chan_count - 1 + 1)
    for dz in (2, 6, 1, 7):
        signal(near_sem, {"grid": at_offset(me, 0, dz, me % 2)})
    send_near(0)
    loads[1].wait()
    row_dft(1)
    send_near(1)
    pl.semaphore_wait(near_sem, 4)
    for d in (2, 1, 3):
        signal(ring_sem, {"grid": line_peer(me, d)})
    for k in (0, 1):
        send_all(k, 6, far_peer)
    for k in (0, 1):
        keep_own(k)
    pl.semaphore_wait(ring_sem, 3)
    for k in (0, 1):
        send_all(k, 48, other_peer)

    received = 0
    for k in range(2, chunks - TAIL):
        while STARTS[k] - STARTS[received] >= AHEAD:
            col_dft(received)
            received += 1
        loads[k].wait()
        row_dft(k)
        send_chunk(k)
    for k in range(chunks - TAIL, chunks):
        loads[k].wait()
        row_dft(k)
    send_tail(range(chunks - TAIL, chunks))
    for k in range(received, chunks):
        col_dft(k)

    power[:NROW] = power[:NROW] + power[NROW:]
    copies = []
    for d in (2, 1, 3):
        peer = lax.rem(group + d, chan_count)
        copies.append(
            pltpu.make_async_remote_copy(
                src_ref=power.at[pl.ds(pl.multiple_of(peer * share, share), share)],
                dst_ref=parts.at[d - 1],
                send_sem=part_send.at[d - 1],
                recv_sem=part_recv.at[d - 1],
                device_id={"chan": peer},
                device_id_type=MESH,
            )
        )
        copies[-1].start()
    for k in range(chunks):
        all_copies(k).wait_send()
    for copy in copies:
        copy.wait()
    total = power[pl.ds(pl.multiple_of(group * share, share), share)]
    total = (total + parts[0]) + (parts[1] + parts[2])
    out[...] = jnp.sum(total.T, axis=0, keepdims=True) * (1.0 / (TIMES * CHANNELS * NROW * GRID_COLUMNS))


def on_device(volt, placement, flags):
    chan_count = lax.axis_size("chan")
    share = NROW // chan_count
    hbm = pl.BlockSpec(memory_space=pltpu.HBM)
    vmem = pl.BlockSpec(memory_space=pltpu.VMEM)
    image = pl.pallas_call(
        kernel,
        name="sky",
        out_shape=pltpu.VMEM((1, share), jnp.float32),
        in_specs=[hbm, hbm, hbm, hbm],
        out_specs=vmem,
        scratch_shapes=[
            pltpu.VMEM((2, TIMES, GRID_COLUMNS, LANES), jnp.float32),
            pltpu.VMEM((2 * TIMES, GRID_COLUMNS, LANES), jnp.float32),
            pltpu.VMEM((2 * TIMES, NROW, LANES), jnp.float32),
            pltpu.VMEM((2 * NROW, 2 * NROW), jnp.float32),
            pltpu.VMEM((1, GRID_COLUMNS), jnp.int32),
            pltpu.VMEM((1, GRID_COLUMNS), jnp.int32),
            pltpu.VMEM((2 * GRID_COLUMNS, 2 * GRID_COLUMNS), jnp.float32),
            pltpu.VMEM((2 * NROW, LANES), jnp.float32),
            pltpu.VMEM((chan_count - 1, share, LANES), jnp.float32),
            pltpu.SemaphoreType.DMA((len(SIZES),)),
            pltpu.SemaphoreType.DMA((3,)),
            pltpu.SemaphoreType.DMA((len(SIZES),)),
            pltpu.SemaphoreType.DMA((len(SIZES),)),
            pltpu.SemaphoreType.REGULAR,
            pltpu.SemaphoreType.REGULAR,
            pltpu.SemaphoreType.DMA((chan_count - 1,)),
            pltpu.SemaphoreType.DMA((chan_count - 1,)),
        ],
        compiler_params=pltpu.CompilerParams(
            collective_id=0, has_side_effects=True, vmem_limit_bytes=60 * 2**20
        ),
    )(
        volt,
        placement.reshape(1, GRID_COLUMNS),
        flags.reshape(1, GRID_COLUMNS),
        jnp.asarray(fourier_matrix()),
    )
    return image.reshape(share, 1)


def solution(mesh):
    return jax.shard_map(
        on_device,
        mesh=mesh,
        in_specs=(P(None, None, "grid", "chan"), P("grid"), P("grid")),
        out_specs=P("chan", "grid"),
        check_vma=False,
    )
```

```python
import math

import jax
import jax.numpy as jnp
import numpy as np
from jax import lax
from jax.experimental import pallas as pl
from jax.experimental.pallas import tpu as pltpu
from jax.sharding import PartitionSpec as P

NROW = 64
GRID_COLUMNS = 64
CHANNELS = 512
TIMES = 128
LANES = 128
SIZES = (8, 8, 16, 16, 16, 16, 16, 16, 8, 4, 2, 2)
STARTS = tuple(sum(SIZES[:k]) for k in range(len(SIZES)))
AHEAD = 64
TAIL = 3
UNROLL = 8
MESH = pl.DeviceIdType.MESH
HIGHEST = lax.Precision.HIGHEST


def fourier_matrix():
    ids = np.outer(np.arange(NROW), np.arange(NROW)) % NROW
    turned = ids * (2.0 * math.pi / NROW)
    cos, sin = np.cos(turned), np.sin(turned)
    return np.block([[cos, sin], [-sin, cos]]).astype(np.float32)


def at_offset(me, dx, dz, core):
    x, z = me // 16, (me // 2) % 8
    return ((x + dx) % 4) * 16 + ((z + dz) % 8) * 2 + core


def near_peer(me, j):
    rank = j // 2
    return at_offset(me, 0, 2 - rank - rank // 2, j % 2)


def far_peer(me, j):
    return at_offset(me, 0, 3 + j // 2, j % 2)


def core_mate(me):
    return me + 1 - 2 * (me % 2)


def other_peer(me, j):
    rank = j // 6
    half = (rank + 1) // 2
    return at_offset(me, 3 - j % 3, 4 + half * (1 - 2 * (rank % 2)), (j // 3) % 2)


def tail_far_peer(me, j):
    rank = j // 8
    return at_offset(me, 3 - j % 4, 4 + (rank + 1) // 2 * (1 - 2 * (rank % 2)), (j // 4) % 2)


def tail_near_peer(me, j, core):
    rank = j // 4
    return at_offset(me, 3 - j % 4, (2 - rank // 2) * (1 - 2 * (rank % 2)), core)


def starts_early(peer):
    return (peer // 16 < 2) & (peer % 2 == 1)


def early_peer(me, j):
    rank = j % 8
    z = (me // 2) % 8 + 4 + (rank + 1) // 2 * (1 - 2 * (rank % 2))
    return j // 8 * 16 + z % 8 * 2 + 1


def line_peer(me, d):
    return (me + 16 * d) % 64


def kernel(
    volt, placement, flags, table, out,
    staged, rows, cols, table_here, placement_here, flags_here, mix, power, parts,
    load_sem, small_sem, send_sem, recv_sem, near_sem, ring_sem, part_send, part_recv,
):
    me = lax.axis_index("grid")
    group = lax.axis_index("chan")
    chan_count = parts.shape[0] + 1
    share = parts.shape[1]
    chunks = len(SIZES)

    def signal(semaphore, peer):
        pl.semaphore_signal(semaphore, inc=1, device_id=peer, device_id_type=MESH)

    loads = [
        pltpu.make_async_copy(
            volt.at[:, pl.ds(STARTS[k], SIZES[k])], staged.at[:, pl.ds(STARTS[k], SIZES[k])], load_sem.at[k]
        )
        for k in range(chunks)
    ]
    small = [
        pltpu.make_async_copy(placement, placement_here, small_sem.at[0]),
        pltpu.make_async_copy(flags, flags_here, small_sem.at[1]),
        pltpu.make_async_copy(table, table_here, small_sem.at[2]),
    ]
    for load in small:
        load.start()

    barrier = pltpu.get_barrier_semaphore()
    for j in range(8):
        signal(barrier, {"grid": near_peer(me, j)})
    for d in (2, 1, 3):
        signal(barrier, {"grid": line_peer(me, d)})
        signal(barrier, {"chan": lax.rem(group + d, chan_count)})
    signal(barrier, {"grid": core_mate(me)})

    for load in loads[:2]:
        load.start()
    for load in small:
        load.wait()

    position = lax.broadcasted_iota(jnp.int32, (GRID_COLUMNS, GRID_COLUMNS), 0)
    pick = jnp.where(position == placement_here[...], flags_here[...].astype(jnp.float32), 0.0)
    none = jnp.zeros_like(pick)
    pick = jnp.concatenate(
        [jnp.concatenate([pick, none], axis=1), jnp.concatenate([none, pick], axis=1)], axis=0
    )
    mix[...] = jnp.dot(table_here[...], pick, precision=HIGHEST, preferred_element_type=jnp.float32)
    power[...] = jnp.zeros_like(power)

    def row_dft(k):
        def one_time(i, carry):
            t = STARTS[k] + i
            x = staged[:, t].reshape(2 * GRID_COLUMNS, LANES)
            y = jnp.dot(mix[...], x, precision=HIGHEST, preferred_element_type=jnp.float32)
            rows[2 * t] = y[:GRID_COLUMNS]
            rows[2 * t + 1] = y[GRID_COLUMNS:]
            return carry

        lax.fori_loop(0, SIZES[k], one_time, 0)

    def span(k):
        return pl.ds(2 * STARTS[k], 2 * SIZES[k])

    def send_to(k, peer):
        pltpu.make_async_remote_copy(
            src_ref=rows.at[span(k), peer],
            dst_ref=cols.at[span(k), me],
            send_sem=send_sem.at[k],
            recv_sem=recv_sem.at[k],
            device_id={"grid": peer},
            device_id_type=MESH,
        ).start()

    def send_all(k, count, peer_at):
        def one_peer(j, carry):
            send_to(k, peer_at(me, j))
            return carry

        lax.fori_loop(0, count, one_peer, 0, unroll=UNROLL)

    def send_near(k):
        send_all(k, 8, near_peer)
        send_to(k, core_mate(me))

    def send_chunk(k):
        send_all(k, 6, far_peer)
        send_near(k)
        send_all(k, 48, other_peer)
        keep_own(k)

    def send_tail(ks):
        def send_if(k, peer, wanted):
            @pl.when(wanted)
            def _():
                send_to(k, peer)

        def send_far(k):
            def one_pair(j, carry):
                early = early_peer(me, j)
                send_if(k, early, early // 2 != me // 2)
                far = tail_far_peer(me, j)
                send_if(k, far, jnp.logical_not(starts_early(far)))
                return carry

            def one_far(j, carry):
                far = tail_far_peer(me, j)
                send_if(k, far, jnp.logical_not(starts_early(far)))
                return carry

            lax.fori_loop(0, 16, one_pair, 0, unroll=UNROLL)
            lax.fori_loop(16, 24, one_far, 0, unroll=UNROLL)

        def send_rest(k, core):
            def one_peer(j, carry):
                near = tail_near_peer(me, j, core)
                send_if(k, near, jnp.logical_not(starts_early(near)))
                return carry

            lax.fori_loop(0, 19, one_peer, 0, unroll=UNROLL)

        for k in ks:
            send_far(k)
        for k in ks:
            send_to(k, core_mate(me))
            keep_own(k)
        for k in ks:
            send_all(k, 19, lambda me, j: tail_near_peer(me, j, 0))
        for k in ks:
            send_rest(k, 1)

    def keep_own(k):
        cols[span(k), pl.ds(me, 1)] = rows[span(k), pl.ds(me, 1)]

    def all_copies(k):
        return pltpu.make_async_remote_copy(
            src_ref=rows.at[span(k), pl.ds(0, NROW - 1)],
            dst_ref=cols.at[span(k), pl.ds(0, NROW - 1)],
            send_sem=send_sem.at[k],
            recv_sem=recv_sem.at[k],
            device_id={"grid": line_peer(me, 1)},
            device_id_type=MESH,
        )

    def col_dft(k):
        all_copies(k).wait_recv()

        def one_time(i, total):
            x = cols[pl.ds(2 * (STARTS[k] + i), 2)].reshape(2 * NROW, LANES)
            y = jnp.dot(table_here[...], x, precision=HIGHEST, preferred_element_type=jnp.float32)
            return total + y * y

        power[...] += lax.fori_loop(0, SIZES[k], one_time, jnp.zeros((2 * NROW, LANES), jnp.float32))

    loads[0].wait()
    for load in loads[2:]:
        load.start()
    row_dft(0)
    pl.semaphore_wait(barrier, 8 + 3 + chan_count - 1 + 1)
    for dz in (2, 6, 1, 7):
        signal(near_sem, {"grid": at_offset(me, 0, dz, me % 2)})
    send_near(0)
    loads[1].wait()
    row_dft(1)
    send_near(1)
    pl.semaphore_wait(near_sem, 4)
    for d in (2, 1, 3):
        signal(ring_sem, {"grid": line_peer(me, d)})
    for k in (0, 1):
        send_all(k, 6, far_peer)
    for k in (0, 1):
        keep_own(k)
    pl.semaphore_wait(ring_sem, 3)
    for k in (0, 1):
        send_all(k, 48, other_peer)

    received = 0
    for k in range(2, chunks - TAIL):
        while STARTS[k] - STARTS[received] >= AHEAD:
            col_dft(received)
            received += 1
        loads[k].wait()
        row_dft(k)
        send_chunk(k)
    for k in range(chunks - TAIL, chunks):
        loads[k].wait()
        row_dft(k)
    send_tail(range(chunks - TAIL, chunks))
    for k in range(received, chunks):
        col_dft(k)

    power[:NROW] = power[:NROW] + power[NROW:]
    copies = []
    for d in (2, 1, 3):
        peer = lax.rem(group + d, chan_count)
        copies.append(
            pltpu.make_async_remote_copy(
                src_ref=power.at[pl.ds(pl.multiple_of(peer * share, share), share)],
                dst_ref=parts.at[d - 1],
                send_sem=part_send.at[d - 1],
                recv_sem=part_recv.at[d - 1],
                device_id={"chan": peer},
                device_id_type=MESH,
            )
        )
        copies[-1].start()
    for k in range(chunks):
        all_copies(k).wait_send()
    for copy in copies:
        copy.wait()
    total = power[pl.ds(pl.multiple_of(group * share, share), share)]
    total = (total + parts[0]) + (parts[1] + parts[2])
    out[...] = jnp.sum(total.T, axis=0, keepdims=True) * (1.0 / (TIMES * CHANNELS * NROW * GRID_COLUMNS))


def on_device(volt, placement, flags):
    chan_count = lax.axis_size("chan")
    share = NROW // chan_count
    hbm = pl.BlockSpec(memory_space=pltpu.HBM)
    vmem = pl.BlockSpec(memory_space=pltpu.VMEM)
    image = pl.pallas_call(
        kernel,
        name="sky",
        out_shape=pltpu.VMEM((1, share), jnp.float32),
        in_specs=[hbm, hbm, hbm, hbm],
        out_specs=vmem,
        scratch_shapes=[
            pltpu.VMEM((2, TIMES, GRID_COLUMNS, LANES), jnp.float32),
            pltpu.VMEM((2 * TIMES, GRID_COLUMNS, LANES), jnp.float32),
            pltpu.VMEM((2 * TIMES, NROW, LANES), jnp.float32),
            pltpu.VMEM((2 * NROW, 2 * NROW), jnp.float32),
            pltpu.VMEM((1, GRID_COLUMNS), jnp.int32),
            pltpu.VMEM((1, GRID_COLUMNS), jnp.int32),
            pltpu.VMEM((2 * GRID_COLUMNS, 2 * GRID_COLUMNS), jnp.float32),
            pltpu.VMEM((2 * NROW, LANES), jnp.float32),
            pltpu.VMEM((chan_count - 1, share, LANES), jnp.float32),
            pltpu.SemaphoreType.DMA((len(SIZES),)),
            pltpu.SemaphoreType.DMA((3,)),
            pltpu.SemaphoreType.DMA((len(SIZES),)),
            pltpu.SemaphoreType.DMA((len(SIZES),)),
            pltpu.SemaphoreType.REGULAR,
            pltpu.SemaphoreType.REGULAR,
            pltpu.SemaphoreType.DMA((chan_count - 1,)),
            pltpu.SemaphoreType.DMA((chan_count - 1,)),
        ],
        compiler_params=pltpu.CompilerParams(
            collective_id=0, has_side_effects=True, vmem_limit_bytes=60 * 2**20
        ),
    )(
        volt,
        placement.reshape(1, GRID_COLUMNS),
        flags.reshape(1, GRID_COLUMNS),
        jnp.asarray(fourier_matrix()),
    )
    return image.reshape(share, 1)


def solution(mesh):
    return jax.shard_map(
        on_device,
        mesh=mesh,
        in_specs=(P(None, None, "grid", "chan"), P("grid"), P("grid")),
        out_specs=P("chan", "grid"),
        check_vma=False,
    )
```

```python
import math

import jax
import jax.numpy as jnp
import numpy as np
from jax import lax
from jax.experimental import pallas as pl
from jax.experimental.pallas import tpu as pltpu
from jax.sharding import PartitionSpec as P

NROW = 64
GRID_COLUMNS = 64
CHANNELS = 512
TIMES = 128
LANES = 128
SIZES = (8, 8, 16, 16, 16, 16, 16, 16, 8, 4, 2, 2)
STARTS = tuple(sum(SIZES[:k]) for k in range(len(SIZES)))
AHEAD = 64
TAIL = 3
UNROLL = 8
MESH = pl.DeviceIdType.MESH
HIGHEST = lax.Precision.HIGHEST


def fourier_matrix():
    ids = np.outer(np.arange(NROW), np.arange(NROW)) % NROW
    turned = ids * (2.0 * math.pi / NROW)
    cos, sin = np.cos(turned), np.sin(turned)
    return np.block([[cos, sin], [-sin, cos]]).astype(np.float32)


def at_offset(me, dx, dz, core):
    x, z = me // 16, (me // 2) % 8
    return ((x + dx) % 4) * 16 + ((z + dz) % 8) * 2 + core


def near_peer(me, j):
    rank = j // 2
    return at_offset(me, 0, 2 - rank - rank // 2, j % 2)


def far_peer(me, j):
    return at_offset(me, 0, 3 + j // 2, j % 2)


def core_mate(me):
    return me + 1 - 2 * (me % 2)


def other_peer(me, j):
    rank = j // 6
    half = (rank + 1) // 2
    return at_offset(me, 3 - j % 3, 4 + half * (1 - 2 * (rank % 2)), (j // 3) % 2)


def tail_far_peer(me, j):
    rank = j // 8
    return at_offset(me, 3 - j % 4, 4 + (rank + 1) // 2 * (1 - 2 * (rank % 2)), (j // 4) % 2)


def tail_near_peer(me, j, core):
    rank = j // 4
    return at_offset(me, 3 - j % 4, (2 - rank // 2) * (1 - 2 * (rank % 2)), core)


def low_x(peer):
    return peer // 16 < 2


def starts_early(peer):
    return low_x(peer) & (peer % 2 == 1)


def early_peer(me, j):
    rank = j % 8
    z = (me // 2) % 8 + 4 + (rank + 1) // 2 * (1 - 2 * (rank % 2))
    return j // 8 * 16 + z % 8 * 2 + 1


def line_peer(me, d):
    return (me + 16 * d) % 64


def kernel(
    volt, placement, flags, table, out,
    staged, rows, cols, table_here, placement_here, flags_here, mix, power, parts,
    load_sem, small_sem, send_sem, recv_sem, near_sem, ring_sem, part_send, part_recv,
):
    me = lax.axis_index("grid")
    group = lax.axis_index("chan")
    chan_count = parts.shape[0] + 1
    share = parts.shape[1]
    chunks = len(SIZES)

    def signal(semaphore, peer):
        pl.semaphore_signal(semaphore, inc=1, device_id=peer, device_id_type=MESH)

    loads = [
        pltpu.make_async_copy(
            volt.at[:, pl.ds(STARTS[k], SIZES[k])], staged.at[:, pl.ds(STARTS[k], SIZES[k])], load_sem.at[k]
        )
        for k in range(chunks)
    ]
    small = [
        pltpu.make_async_copy(placement, placement_here, small_sem.at[0]),
        pltpu.make_async_copy(flags, flags_here, small_sem.at[1]),
        pltpu.make_async_copy(table, table_here, small_sem.at[2]),
    ]
    for load in small:
        load.start()

    barrier = pltpu.get_barrier_semaphore()
    for j in range(8):
        signal(barrier, {"grid": near_peer(me, j)})
    for d in (2, 1, 3):
        signal(barrier, {"grid": line_peer(me, d)})
        signal(barrier, {"chan": lax.rem(group + d, chan_count)})
    signal(barrier, {"grid": core_mate(me)})

    for load in loads[:2]:
        load.start()
    for load in small:
        load.wait()

    position = lax.broadcasted_iota(jnp.int32, (GRID_COLUMNS, GRID_COLUMNS), 0)
    pick = jnp.where(position == placement_here[...], flags_here[...].astype(jnp.float32), 0.0)
    none = jnp.zeros_like(pick)
    pick = jnp.concatenate(
        [jnp.concatenate([pick, none], axis=1), jnp.concatenate([none, pick], axis=1)], axis=0
    )
    mix[...] = jnp.dot(table_here[...], pick, precision=HIGHEST, preferred_element_type=jnp.float32)
    power[...] = jnp.zeros_like(power)

    def row_dft(k):
        def one_time(i, carry):
            t = STARTS[k] + i
            x = staged[:, t].reshape(2 * GRID_COLUMNS, LANES)
            y = jnp.dot(mix[...], x, precision=HIGHEST, preferred_element_type=jnp.float32)
            rows[2 * t] = y[:GRID_COLUMNS]
            rows[2 * t + 1] = y[GRID_COLUMNS:]
            return carry

        lax.fori_loop(0, SIZES[k], one_time, 0)

    def span(k):
        return pl.ds(2 * STARTS[k], 2 * SIZES[k])

    def send_to(k, peer):
        pltpu.make_async_remote_copy(
            src_ref=rows.at[span(k), peer],
            dst_ref=cols.at[span(k), me],
            send_sem=send_sem.at[k],
            recv_sem=recv_sem.at[k],
            device_id={"grid": peer},
            device_id_type=MESH,
        ).start()

    def send_all(k, count, peer_at):
        def one_peer(j, carry):
            send_to(k, peer_at(me, j))
            return carry

        lax.fori_loop(0, count, one_peer, 0, unroll=UNROLL)

    def send_near(k):
        send_all(k, 8, near_peer)
        send_to(k, core_mate(me))

    def send_chunk(k):
        send_all(k, 6, far_peer)
        send_near(k)
        send_all(k, 48, other_peer)
        keep_own(k)

    def send_tail(ks):
        def send_if(k, peer, wanted):
            @pl.when(wanted)
            def _():
                send_to(k, peer)

        def send_far(k):
            def one_pair(j, carry):
                early = early_peer(me, j)
                send_if(k, early, early // 2 != me // 2)
                far = tail_far_peer(me, j)
                send_if(k, far, jnp.logical_not(starts_early(far)))
                return carry

            def one_far(j, carry):
                far = tail_far_peer(me, j)
                send_if(k, far, jnp.logical_not(starts_early(far)))
                return carry

            lax.fori_loop(0, 16, one_pair, 0, unroll=UNROLL)
            lax.fori_loop(16, 24, one_far, 0, unroll=UNROLL)

        def send_rest(k, core, low):
            def one_peer(j, carry):
                near = tail_near_peer(me, j, core)
                send_if(k, near, low_x(near) == low)
                return carry

            lax.fori_loop(0, 19, one_peer, 0, unroll=UNROLL)

        for k in ks:
            send_far(k)
        for k in ks:
            send_to(k, core_mate(me))
            keep_own(k)
        for core, low in ((0, True), (0, False), (1, False)):
            for k in ks:
                send_rest(k, core, low)

    def keep_own(k):
        cols[span(k), pl.ds(me, 1)] = rows[span(k), pl.ds(me, 1)]

    def all_copies(k):
        return pltpu.make_async_remote_copy(
            src_ref=rows.at[span(k), pl.ds(0, NROW - 1)],
            dst_ref=cols.at[span(k), pl.ds(0, NROW - 1)],
            send_sem=send_sem.at[k],
            recv_sem=recv_sem.at[k],
            device_id={"grid": line_peer(me, 1)},
            device_id_type=MESH,
        )

    def col_dft(k):
        all_copies(k).wait_recv()

        def one_time(i, total):
            x = cols[pl.ds(2 * (STARTS[k] + i), 2)].reshape(2 * NROW, LANES)
            y = jnp.dot(table_here[...], x, precision=HIGHEST, preferred_element_type=jnp.float32)
            return total + y * y

        power[...] += lax.fori_loop(0, SIZES[k], one_time, jnp.zeros((2 * NROW, LANES), jnp.float32))

    loads[0].wait()
    for load in loads[2:]:
        load.start()
    row_dft(0)
    pl.semaphore_wait(barrier, 8 + 3 + chan_count - 1 + 1)
    for dz in (2, 6, 1, 7):
        signal(near_sem, {"grid": at_offset(me, 0, dz, me % 2)})
    send_near(0)
    loads[1].wait()
    row_dft(1)
    send_near(1)
    pl.semaphore_wait(near_sem, 4)
    for d in (2, 1, 3):
        signal(ring_sem, {"grid": line_peer(me, d)})
    for k in (0, 1):
        send_all(k, 6, far_peer)
    for k in (0, 1):
        keep_own(k)
    pl.semaphore_wait(ring_sem, 3)
    for k in (0, 1):
        send_all(k, 48, other_peer)

    received = 0
    for k in range(2, chunks - TAIL):
        while STARTS[k] - STARTS[received] >= AHEAD:
            col_dft(received)
            received += 1
        loads[k].wait()
        row_dft(k)
        send_chunk(k)
    for k in range(chunks - TAIL, chunks):
        loads[k].wait()
        row_dft(k)
    send_tail(range(chunks - TAIL, chunks))
    for k in range(received, chunks):
        col_dft(k)

    power[:NROW] = power[:NROW] + power[NROW:]
    copies = []
    for d in (2, 1, 3):
        peer = lax.rem(group + d, chan_count)
        copies.append(
            pltpu.make_async_remote_copy(
                src_ref=power.at[pl.ds(pl.multiple_of(peer * share, share), share)],
                dst_ref=parts.at[d - 1],
                send_sem=part_send.at[d - 1],
                recv_sem=part_recv.at[d - 1],
                device_id={"chan": peer},
                device_id_type=MESH,
            )
        )
        copies[-1].start()
    for k in range(chunks):
        all_copies(k).wait_send()
    for copy in copies:
        copy.wait()
    total = power[pl.ds(pl.multiple_of(group * share, share), share)]
    total = (total + parts[0]) + (parts[1] + parts[2])
    out[...] = jnp.sum(total.T, axis=0, keepdims=True) * (1.0 / (TIMES * CHANNELS * NROW * GRID_COLUMNS))


def on_device(volt, placement, flags):
    chan_count = lax.axis_size("chan")
    share = NROW // chan_count
    hbm = pl.BlockSpec(memory_space=pltpu.HBM)
    vmem = pl.BlockSpec(memory_space=pltpu.VMEM)
    image = pl.pallas_call(
        kernel,
        name="sky",
        out_shape=pltpu.VMEM((1, share), jnp.float32),
        in_specs=[hbm, hbm, hbm, hbm],
        out_specs=vmem,
        scratch_shapes=[
            pltpu.VMEM((2, TIMES, GRID_COLUMNS, LANES), jnp.float32),
            pltpu.VMEM((2 * TIMES, GRID_COLUMNS, LANES), jnp.float32),
            pltpu.VMEM((2 * TIMES, NROW, LANES), jnp.float32),
            pltpu.VMEM((2 * NROW, 2 * NROW), jnp.float32),
            pltpu.VMEM((1, GRID_COLUMNS), jnp.int32),
            pltpu.VMEM((1, GRID_COLUMNS), jnp.int32),
            pltpu.VMEM((2 * GRID_COLUMNS, 2 * GRID_COLUMNS), jnp.float32),
            pltpu.VMEM((2 * NROW, LANES), jnp.float32),
            pltpu.VMEM((chan_count - 1, share, LANES), jnp.float32),
            pltpu.SemaphoreType.DMA((len(SIZES),)),
            pltpu.SemaphoreType.DMA((3,)),
            pltpu.SemaphoreType.DMA((len(SIZES),)),
            pltpu.SemaphoreType.DMA((len(SIZES),)),
            pltpu.SemaphoreType.REGULAR,
            pltpu.SemaphoreType.REGULAR,
            pltpu.SemaphoreType.DMA((chan_count - 1,)),
            pltpu.SemaphoreType.DMA((chan_count - 1,)),
        ],
        compiler_params=pltpu.CompilerParams(
            collective_id=0, has_side_effects=True, vmem_limit_bytes=60 * 2**20
        ),
    )(
        volt,
        placement.reshape(1, GRID_COLUMNS),
        flags.reshape(1, GRID_COLUMNS),
        jnp.asarray(fourier_matrix()),
    )
    return image.reshape(share, 1)


def solution(mesh):
    return jax.shard_map(
        on_device,
        mesh=mesh,
        in_specs=(P(None, None, "grid", "chan"), P("grid"), P("grid")),
        out_specs=P("chan", "grid"),
        check_vma=False,
    )
```

```python
import math

import jax
import jax.numpy as jnp
import numpy as np
from jax import lax
from jax.experimental import pallas as pl
from jax.experimental.pallas import tpu as pltpu
from jax.sharding import PartitionSpec as P

NROW = 64
GRID_COLUMNS = 64
CHANNELS = 512
TIMES = 128
LANES = 128
SIZES = (4, 8, 12, 16, 16, 16, 16, 16, 8, 8, 4, 2, 2)
STARTS = tuple(sum(SIZES[:k]) for k in range(len(SIZES)))
AHEAD = 64
TAIL = 3
UNROLL = 8
MESH = pl.DeviceIdType.MESH
HIGHEST = lax.Precision.HIGHEST


def fourier_matrix():
    ids = np.outer(np.arange(NROW), np.arange(NROW)) % NROW
    turned = ids * (2.0 * math.pi / NROW)
    cos, sin = np.cos(turned), np.sin(turned)
    return np.block([[cos, sin], [-sin, cos]]).astype(np.float32)


def at_offset(me, dx, dz, core):
    x, z = me // 16, (me // 2) % 8
    return ((x + dx) % 4) * 16 + ((z + dz) % 8) * 2 + core


def near_peer(me, j):
    rank = j // 2
    return at_offset(me, 0, 2 - rank - rank // 2, j % 2)


def far_peer(me, j):
    return at_offset(me, 0, 3 + j // 2, j % 2)


def core_mate(me):
    return me + 1 - 2 * (me % 2)


def other_peer(me, j):
    rank = j // 6
    half = (rank + 1) // 2
    return at_offset(me, 3 - j % 3, 4 + half * (1 - 2 * (rank % 2)), (j // 3) % 2)


def tail_far_peer(me, j):
    rank = j // 8
    return at_offset(me, 3 - j % 4, 4 + (rank + 1) // 2 * (1 - 2 * (rank % 2)), (j // 4) % 2)


def tail_near_peer(me, j, core):
    rank = j // 4
    return at_offset(me, 3 - j % 4, (2 - rank // 2) * (1 - 2 * (rank % 2)), core)


def starts_early(peer):
    return (peer // 16 < 2) & (peer % 2 == 1)


def early_peer(me, j):
    rank = j % 8
    z = (me // 2) % 8 + 4 + (rank + 1) // 2 * (1 - 2 * (rank % 2))
    return j // 8 * 16 + z % 8 * 2 + 1


def line_peer(me, d):
    return (me + 16 * d) % 64


def kernel(
    volt, placement, flags, table, out,
    staged, rows, cols, table_here, placement_here, flags_here, mix, power, parts,
    load_sem, small_sem, send_sem, recv_sem, near_sem, ring_sem, part_send, part_recv,
):
    me = lax.axis_index("grid")
    group = lax.axis_index("chan")
    chan_count = parts.shape[0] + 1
    share = parts.shape[1]
    chunks = len(SIZES)

    def signal(semaphore, peer):
        pl.semaphore_signal(semaphore, inc=1, device_id=peer, device_id_type=MESH)

    loads = [
        pltpu.make_async_copy(
            volt.at[:, pl.ds(STARTS[k], SIZES[k])], staged.at[:, pl.ds(STARTS[k], SIZES[k])], load_sem.at[k]
        )
        for k in range(chunks)
    ]
    small = [
        pltpu.make_async_copy(placement, placement_here, small_sem.at[0]),
        pltpu.make_async_copy(flags, flags_here, small_sem.at[1]),
        pltpu.make_async_copy(table, table_here, small_sem.at[2]),
    ]
    for load in small:
        load.start()

    barrier = pltpu.get_barrier_semaphore()
    for j in range(8):
        signal(barrier, {"grid": near_peer(me, j)})
    for d in (2, 1, 3):
        signal(barrier, {"grid": line_peer(me, d)})
        signal(barrier, {"chan": lax.rem(group + d, chan_count)})
    signal(barrier, {"grid": core_mate(me)})

    for load in loads[:2]:
        load.start()
    for load in small:
        load.wait()

    position = lax.broadcasted_iota(jnp.int32, (GRID_COLUMNS, GRID_COLUMNS), 0)
    pick = jnp.where(position == placement_here[...], flags_here[...].astype(jnp.float32), 0.0)
    none = jnp.zeros_like(pick)
    pick = jnp.concatenate(
        [jnp.concatenate([pick, none], axis=1), jnp.concatenate([none, pick], axis=1)], axis=0
    )
    mix[...] = jnp.dot(table_here[...], pick, precision=HIGHEST, preferred_element_type=jnp.float32)
    power[...] = jnp.zeros_like(power)

    def row_dft(k):
        def one_time(i, carry):
            t = STARTS[k] + i
            x = staged[:, t].reshape(2 * GRID_COLUMNS, LANES)
            y = jnp.dot(mix[...], x, precision=HIGHEST, preferred_element_type=jnp.float32)
            rows[2 * t] = y[:GRID_COLUMNS]
            rows[2 * t + 1] = y[GRID_COLUMNS:]
            return carry

        lax.fori_loop(0, SIZES[k], one_time, 0)

    def span(k):
        return pl.ds(2 * STARTS[k], 2 * SIZES[k])

    def send_to(k, peer):
        pltpu.make_async_remote_copy(
            src_ref=rows.at[span(k), peer],
            dst_ref=cols.at[span(k), me],
            send_sem=send_sem.at[k],
            recv_sem=recv_sem.at[k],
            device_id={"grid": peer},
            device_id_type=MESH,
        ).start()

    def send_all(k, count, peer_at):
        def one_peer(j, carry):
            send_to(k, peer_at(me, j))
            return carry

        lax.fori_loop(0, count, one_peer, 0, unroll=UNROLL)

    def send_near(k):
        send_all(k, 8, near_peer)
        send_to(k, core_mate(me))

    def send_chunk(k):
        send_all(k, 6, far_peer)
        send_near(k)
        send_all(k, 48, other_peer)
        keep_own(k)

    def send_tail(ks):
        def send_if(k, peer, wanted):
            @pl.when(wanted)
            def _():
                send_to(k, peer)

        def send_far(k):
            def one_pair(j, carry):
                early = early_peer(me, j)
                send_if(k, early, early // 2 != me // 2)
                far = tail_far_peer(me, j)
                send_if(k, far, jnp.logical_not(starts_early(far)))
                return carry

            def one_far(j, carry):
                far = tail_far_peer(me, j)
                send_if(k, far, jnp.logical_not(starts_early(far)))
                return carry

            lax.fori_loop(0, 16, one_pair, 0, unroll=UNROLL)
            lax.fori_loop(16, 24, one_far, 0, unroll=UNROLL)

        def send_rest(k, core):
            def one_peer(j, carry):
                near = tail_near_peer(me, j, core)
                send_if(k, near, jnp.logical_not(starts_early(near)))
                return carry

            lax.fori_loop(0, 19, one_peer, 0, unroll=UNROLL)

        for k in ks:
            send_far(k)
        for k in ks:
            send_to(k, core_mate(me))
            keep_own(k)
        for k in ks:
            send_all(k, 19, lambda me, j: tail_near_peer(me, j, 0))
        for k in ks:
            send_rest(k, 1)

    def keep_own(k):
        cols[span(k), pl.ds(me, 1)] = rows[span(k), pl.ds(me, 1)]

    def all_copies(k):
        return pltpu.make_async_remote_copy(
            src_ref=rows.at[span(k), pl.ds(0, NROW - 1)],
            dst_ref=cols.at[span(k), pl.ds(0, NROW - 1)],
            send_sem=send_sem.at[k],
            recv_sem=recv_sem.at[k],
            device_id={"grid": line_peer(me, 1)},
            device_id_type=MESH,
        )

    def col_dft(k):
        all_copies(k).wait_recv()

        def one_time(i, total):
            x = cols[pl.ds(2 * (STARTS[k] + i), 2)].reshape(2 * NROW, LANES)
            y = jnp.dot(table_here[...], x, precision=HIGHEST, preferred_element_type=jnp.float32)
            return total + y * y

        power[...] += lax.fori_loop(0, SIZES[k], one_time, jnp.zeros((2 * NROW, LANES), jnp.float32))

    loads[0].wait()
    for load in loads[2:]:
        load.start()
    row_dft(0)
    pl.semaphore_wait(barrier, 8 + 3 + chan_count - 1 + 1)
    for dz in (2, 6, 1, 7):
        signal(near_sem, {"grid": at_offset(me, 0, dz, me % 2)})
    send_near(0)
    loads[1].wait()
    row_dft(1)
    send_near(1)
    pl.semaphore_wait(near_sem, 4)
    for d in (2, 1, 3):
        signal(ring_sem, {"grid": line_peer(me, d)})
    for k in (0, 1):
        send_all(k, 6, far_peer)
    for k in (0, 1):
        keep_own(k)
    pl.semaphore_wait(ring_sem, 3)
    for k in (0, 1):
        send_all(k, 48, other_peer)

    received = 0
    for k in range(2, chunks - TAIL):
        while STARTS[k] - STARTS[received] >= AHEAD:
            col_dft(received)
            received += 1
        loads[k].wait()
        row_dft(k)
        send_chunk(k)
    for k in range(chunks - TAIL, chunks):
        loads[k].wait()
        row_dft(k)
    send_tail(range(chunks - TAIL, chunks))
    for k in range(received, chunks):
        col_dft(k)

    power[:NROW] = power[:NROW] + power[NROW:]
    copies = []
    for d in (2, 1, 3):
        peer = lax.rem(group + d, chan_count)
        copies.append(
            pltpu.make_async_remote_copy(
                src_ref=power.at[pl.ds(pl.multiple_of(peer * share, share), share)],
                dst_ref=parts.at[d - 1],
                send_sem=part_send.at[d - 1],
                recv_sem=part_recv.at[d - 1],
                device_id={"chan": peer},
                device_id_type=MESH,
            )
        )
        copies[-1].start()
    for k in range(chunks):
        all_copies(k).wait_send()
    for copy in copies:
        copy.wait()
    total = power[pl.ds(pl.multiple_of(group * share, share), share)]
    total = (total + parts[0]) + (parts[1] + parts[2])
    out[...] = jnp.sum(total.T, axis=0, keepdims=True) * (1.0 / (TIMES * CHANNELS * NROW * GRID_COLUMNS))


def on_device(volt, placement, flags):
    chan_count = lax.axis_size("chan")
    share = NROW // chan_count
    hbm = pl.BlockSpec(memory_space=pltpu.HBM)
    vmem = pl.BlockSpec(memory_space=pltpu.VMEM)
    image = pl.pallas_call(
        kernel,
        name="sky",
        out_shape=pltpu.VMEM((1, share), jnp.float32),
        in_specs=[hbm, hbm, hbm, hbm],
        out_specs=vmem,
        scratch_shapes=[
            pltpu.VMEM((2, TIMES, GRID_COLUMNS, LANES), jnp.float32),
            pltpu.VMEM((2 * TIMES, GRID_COLUMNS, LANES), jnp.float32),
            pltpu.VMEM((2 * TIMES, NROW, LANES), jnp.float32),
            pltpu.VMEM((2 * NROW, 2 * NROW), jnp.float32),
            pltpu.VMEM((1, GRID_COLUMNS), jnp.int32),
            pltpu.VMEM((1, GRID_COLUMNS), jnp.int32),
            pltpu.VMEM((2 * GRID_COLUMNS, 2 * GRID_COLUMNS), jnp.float32),
            pltpu.VMEM((2 * NROW, LANES), jnp.float32),
            pltpu.VMEM((chan_count - 1, share, LANES), jnp.float32),
            pltpu.SemaphoreType.DMA((len(SIZES),)),
            pltpu.SemaphoreType.DMA((3,)),
            pltpu.SemaphoreType.DMA((len(SIZES),)),
            pltpu.SemaphoreType.DMA((len(SIZES),)),
            pltpu.SemaphoreType.REGULAR,
            pltpu.SemaphoreType.REGULAR,
            pltpu.SemaphoreType.DMA((chan_count - 1,)),
            pltpu.SemaphoreType.DMA((chan_count - 1,)),
        ],
        compiler_params=pltpu.CompilerParams(
            collective_id=0, has_side_effects=True, vmem_limit_bytes=60 * 2**20
        ),
    )(
        volt,
        placement.reshape(1, GRID_COLUMNS),
        flags.reshape(1, GRID_COLUMNS),
        jnp.asarray(fourier_matrix()),
    )
    return image.reshape(share, 1)


def solution(mesh):
    return jax.shard_map(
        on_device,
        mesh=mesh,
        in_specs=(P(None, None, "grid", "chan"), P("grid"), P("grid")),
        out_specs=P("chan", "grid"),
        check_vma=False,
    )
```

```python
import math

import jax
import jax.numpy as jnp
import numpy as np
from jax import lax
from jax.experimental import pallas as pl
from jax.experimental.pallas import tpu as pltpu
from jax.sharding import PartitionSpec as P

NROW = 64
GRID_COLUMNS = 64
CHANNELS = 512
TIMES = 128
LANES = 128
SIZES = (4, 8, 12, 16, 16, 16, 16, 16, 8, 8, 4, 2, 2)
STARTS = tuple(sum(SIZES[:k]) for k in range(len(SIZES)))
AHEAD = 64
TAIL = 3
UNROLL = 8
MESH = pl.DeviceIdType.MESH
HIGHEST = lax.Precision.HIGHEST


def fourier_matrix():
    ids = np.outer(np.arange(NROW), np.arange(NROW)) % NROW
    turned = ids * (2.0 * math.pi / NROW)
    cos, sin = np.cos(turned), np.sin(turned)
    return np.block([[cos, sin], [-sin, cos]]).astype(np.float32)


def at_offset(me, dx, dz, core):
    x, z = me // 16, (me // 2) % 8
    return ((x + dx) % 4) * 16 + ((z + dz) % 8) * 2 + core


def near_peer(me, j):
    rank = j // 2
    return at_offset(me, 0, 2 - rank - rank // 2, j % 2)


def far_peer(me, j):
    return at_offset(me, 0, 3 + j // 2, j % 2)


def core_mate(me):
    return me + 1 - 2 * (me % 2)


def other_peer(me, j):
    rank = j // 6
    half = (rank + 1) // 2
    return at_offset(me, 3 - j % 3, 4 + half * (1 - 2 * (rank % 2)), (j // 3) % 2)


def tail_far_peer(me, j):
    rank = j // 8
    return at_offset(me, 3 - j % 4, 4 + (rank + 1) // 2 * (1 - 2 * (rank % 2)), (j // 4) % 2)


def tail_near_peer(me, j, core):
    rank = j // 4
    return at_offset(me, 3 - j % 4, (2 - rank // 2) * (1 - 2 * (rank % 2)), core)


def starts_early(peer):
    return (peer // 16 < 2) & (peer % 2 == 1)


def early_peer(me, j):
    rank = j % 8
    z = (me // 2) % 8 + 4 + (rank + 1) // 2 * (1 - 2 * (rank % 2))
    return j // 8 * 16 + z % 8 * 2 + 1


def line_peer(me, d):
    return (me + 16 * d) % 64


def kernel(
    volt, placement, flags, table, out,
    staged, rows, cols, table_here, placement_here, flags_here, mix, power, parts,
    load_sem, small_sem, send_sem, recv_sem, near_sem, ring_sem, part_send, part_recv,
):
    me = lax.axis_index("grid")
    group = lax.axis_index("chan")
    chan_count = parts.shape[0] + 1
    share = parts.shape[1]
    chunks = len(SIZES)

    def signal(semaphore, peer):
        pl.semaphore_signal(semaphore, inc=1, device_id=peer, device_id_type=MESH)

    loads = [
        pltpu.make_async_copy(
            volt.at[:, pl.ds(STARTS[k], SIZES[k])], staged.at[:, pl.ds(STARTS[k], SIZES[k])], load_sem.at[k]
        )
        for k in range(chunks)
    ]
    small = [
        pltpu.make_async_copy(placement, placement_here, small_sem.at[0]),
        pltpu.make_async_copy(flags, flags_here, small_sem.at[1]),
        pltpu.make_async_copy(table, table_here, small_sem.at[2]),
    ]
    for load in small:
        load.start()

    barrier = pltpu.get_barrier_semaphore()
    for j in range(8):
        signal(barrier, {"grid": near_peer(me, j)})
    for d in (2, 1, 3):
        signal(barrier, {"grid": line_peer(me, d)})
        signal(barrier, {"chan": lax.rem(group + d, chan_count)})
    signal(barrier, {"grid": core_mate(me)})

    for load in loads[:2]:
        load.start()
    for load in small:
        load.wait()

    position = lax.broadcasted_iota(jnp.int32, (GRID_COLUMNS, GRID_COLUMNS), 0)
    pick = jnp.where(position == placement_here[...], flags_here[...].astype(jnp.float32), 0.0)
    none = jnp.zeros_like(pick)
    pick = jnp.concatenate(
        [jnp.concatenate([pick, none], axis=1), jnp.concatenate([none, pick], axis=1)], axis=0
    )
    mix[...] = jnp.dot(table_here[...], pick, precision=HIGHEST, preferred_element_type=jnp.float32)
    power[...] = jnp.zeros_like(power)

    def row_dft(k):
        def one_time(i, carry):
            t = STARTS[k] + i
            x = staged[:, t].reshape(2 * GRID_COLUMNS, LANES)
            y = jnp.dot(mix[...], x, precision=HIGHEST, preferred_element_type=jnp.float32)
            rows[2 * t] = y[:GRID_COLUMNS]
            rows[2 * t + 1] = y[GRID_COLUMNS:]
            return carry

        lax.fori_loop(0, SIZES[k], one_time, 0, unroll=2)

    def span(k):
        return pl.ds(2 * STARTS[k], 2 * SIZES[k])

    def send_to(k, peer):
        pltpu.make_async_remote_copy(
            src_ref=rows.at[span(k), peer],
            dst_ref=cols.at[span(k), me],
            send_sem=send_sem.at[k],
            recv_sem=recv_sem.at[k],
            device_id={"grid": peer},
            device_id_type=MESH,
        ).start()

    def send_all(k, count, peer_at):
        def one_peer(j, carry):
            send_to(k, peer_at(me, j))
            return carry

        lax.fori_loop(0, count, one_peer, 0, unroll=UNROLL)

    def send_near(k):
        send_all(k, 8, near_peer)
        send_to(k, core_mate(me))

    def send_chunk(k):
        send_all(k, 6, far_peer)
        send_near(k)
        send_all(k, 48, other_peer)
        keep_own(k)

    def send_tail(ks):
        def send_if(k, peer, wanted):
            @pl.when(wanted)
            def _():
                send_to(k, peer)

        def send_far(k):
            def one_pair(j, carry):
                early = early_peer(me, j)
                send_if(k, early, early // 2 != me // 2)
                far = tail_far_peer(me, j)
                send_if(k, far, jnp.logical_not(starts_early(far)))
                return carry

            def one_far(j, carry):
                far = tail_far_peer(me, j)
                send_if(k, far, jnp.logical_not(starts_early(far)))
                return carry

            lax.fori_loop(0, 16, one_pair, 0, unroll=UNROLL)
            lax.fori_loop(16, 24, one_far, 0, unroll=UNROLL)

        def send_rest(k, core):
            def one_peer(j, carry):
                near = tail_near_peer(me, j, core)
                send_if(k, near, jnp.logical_not(starts_early(near)))
                return carry

            lax.fori_loop(0, 19, one_peer, 0, unroll=UNROLL)

        for k in ks:
            send_far(k)
        for k in ks:
            send_to(k, core_mate(me))
            keep_own(k)
        for k in ks:
            send_all(k, 19, lambda me, j: tail_near_peer(me, j, 0))
        for k in ks:
            send_rest(k, 1)

    def keep_own(k):
        cols[span(k), pl.ds(me, 1)] = rows[span(k), pl.ds(me, 1)]

    def all_copies(k):
        return pltpu.make_async_remote_copy(
            src_ref=rows.at[span(k), pl.ds(0, NROW - 1)],
            dst_ref=cols.at[span(k), pl.ds(0, NROW - 1)],
            send_sem=send_sem.at[k],
            recv_sem=recv_sem.at[k],
            device_id={"grid": line_peer(me, 1)},
            device_id_type=MESH,
        )

    def col_dft(k):
        all_copies(k).wait_recv()

        def one_time(i, total):
            x = cols[pl.ds(2 * (STARTS[k] + i), 2)].reshape(2 * NROW, LANES)
            y = jnp.dot(table_here[...], x, precision=HIGHEST, preferred_element_type=jnp.float32)
            return total + y * y

        power[...] += lax.fori_loop(0, SIZES[k], one_time, jnp.zeros((2 * NROW, LANES), jnp.float32), unroll=2)

    loads[0].wait()
    for load in loads[2:]:
        load.start()
    row_dft(0)
    pl.semaphore_wait(barrier, 8 + 3 + chan_count - 1 + 1)
    for dz in (2, 6, 1, 7):
        signal(near_sem, {"grid": at_offset(me, 0, dz, me % 2)})
    send_near(0)
    loads[1].wait()
    row_dft(1)
    send_near(1)
    pl.semaphore_wait(near_sem, 4)
    for d in (2, 1, 3):
        signal(ring_sem, {"grid": line_peer(me, d)})
    for k in (0, 1):
        send_all(k, 6, far_peer)
    for k in (0, 1):
        keep_own(k)
    pl.semaphore_wait(ring_sem, 3)
    for k in (0, 1):
        send_all(k, 48, other_peer)

    received = 0
    for k in range(2, chunks - TAIL):
        while STARTS[k] - STARTS[received] >= AHEAD:
            col_dft(received)
            received += 1
        loads[k].wait()
        row_dft(k)
        send_chunk(k)
    for k in range(chunks - TAIL, chunks):
        loads[k].wait()
        row_dft(k)
    send_tail(range(chunks - TAIL, chunks))
    for k in range(received, chunks):
        col_dft(k)

    power[:NROW] = power[:NROW] + power[NROW:]
    copies = []
    for d in (2, 1, 3):
        peer = lax.rem(group + d, chan_count)
        copies.append(
            pltpu.make_async_remote_copy(
                src_ref=power.at[pl.ds(pl.multiple_of(peer * share, share), share)],
                dst_ref=parts.at[d - 1],
                send_sem=part_send.at[d - 1],
                recv_sem=part_recv.at[d - 1],
                device_id={"chan": peer},
                device_id_type=MESH,
            )
        )
        copies[-1].start()
    for k in range(chunks):
        all_copies(k).wait_send()
    for copy in copies:
        copy.wait()
    total = power[pl.ds(pl.multiple_of(group * share, share), share)]
    total = (total + parts[0]) + (parts[1] + parts[2])
    out[...] = jnp.sum(total.T, axis=0, keepdims=True) * (1.0 / (TIMES * CHANNELS * NROW * GRID_COLUMNS))


def on_device(volt, placement, flags):
    chan_count = lax.axis_size("chan")
    share = NROW // chan_count
    hbm = pl.BlockSpec(memory_space=pltpu.HBM)
    vmem = pl.BlockSpec(memory_space=pltpu.VMEM)
    image = pl.pallas_call(
        kernel,
        name="sky",
        out_shape=pltpu.VMEM((1, share), jnp.float32),
        in_specs=[hbm, hbm, hbm, hbm],
        out_specs=vmem,
        scratch_shapes=[
            pltpu.VMEM((2, TIMES, GRID_COLUMNS, LANES), jnp.float32),
            pltpu.VMEM((2 * TIMES, GRID_COLUMNS, LANES), jnp.float32),
            pltpu.VMEM((2 * TIMES, NROW, LANES), jnp.float32),
            pltpu.VMEM((2 * NROW, 2 * NROW), jnp.float32),
            pltpu.VMEM((1, GRID_COLUMNS), jnp.int32),
            pltpu.VMEM((1, GRID_COLUMNS), jnp.int32),
            pltpu.VMEM((2 * GRID_COLUMNS, 2 * GRID_COLUMNS), jnp.float32),
            pltpu.VMEM((2 * NROW, LANES), jnp.float32),
            pltpu.VMEM((chan_count - 1, share, LANES), jnp.float32),
            pltpu.SemaphoreType.DMA((len(SIZES),)),
            pltpu.SemaphoreType.DMA((3,)),
            pltpu.SemaphoreType.DMA((len(SIZES),)),
            pltpu.SemaphoreType.DMA((len(SIZES),)),
            pltpu.SemaphoreType.REGULAR,
            pltpu.SemaphoreType.REGULAR,
            pltpu.SemaphoreType.DMA((chan_count - 1,)),
            pltpu.SemaphoreType.DMA((chan_count - 1,)),
        ],
        compiler_params=pltpu.CompilerParams(
            collective_id=0, has_side_effects=True, vmem_limit_bytes=60 * 2**20
        ),
    )(
        volt,
        placement.reshape(1, GRID_COLUMNS),
        flags.reshape(1, GRID_COLUMNS),
        jnp.asarray(fourier_matrix()),
    )
    return image.reshape(share, 1)


def solution(mesh):
    return jax.shard_map(
        on_device,
        mesh=mesh,
        in_specs=(P(None, None, "grid", "chan"), P("grid"), P("grid")),
        out_specs=P("chan", "grid"),
        check_vma=False,
    )
```
